32 devices in a mesh: data: 1 (over z), col: 4 (over y), row: 8 (over x, core).
Axes of the slice: x: 4, y: 4, z: 1, core: 2. Of those that a mesh axis runs over, the one named last changes fastest.
The devices are a block of a 4x4x8 slice.
Arguments:
- seq_in: bfloat16 [16, 8, 2816], P(None, 'data', 'row')
- w_x1: bfloat16 [2816, 11264], P('row', 'col')
- w_h1: bfloat16 [2816, 11264], P('row', 'col')
- w_x2: bfloat16 [2816, 11264], P('row', 'col')
- w_h2: bfloat16 [2816, 11264], P('row', 'col')
- bias_1: float32 [11264], P('col')
- bias_2: float32 [11264], P('col')
- h_init: float32 [2, 8, 2816], P(None, 'data', 'row')
- c_init: float32 [2, 8, 2816], P(None, 'data', 'row')
- g_out: bfloat16 [16, 8, 2816], P(None, 'data', 'col')
Outputs:
- output 1: float32 [2816, 11264], P(('data', 'row'), 'col')
- output 2: float32 [2816, 11264], P(('data', 'row'), 'col')
- output 3: float32 [2816, 11264], P(('data', 'row'), 'col')
- output 4: float32 [2816, 11264], P(('data', 'row'), 'col')
- output 5: float32 [11264], P(('data', 'col'))
- output 6: float32 [11264], P(('data', 'col'))
All inputs are finite; a program needn't handle non-finite values.
Results may differ from the reference program's by a relative error of at most 0.0062514.
Values are sent between devices in bfloat16 or wider.
A program may use at most 768 MiB of HBM per device.

```python
import jax
import jax.numpy as jnp
from jax import lax

SEQ_LEN = 16
GROUP_BATCH = 8
HIDDEN = 2816


def setup_inputs(seed: int = 0, part: int = 0) -> dict:
    root_key = jax.random.key(seed)
    shared_keys = jax.random.split(root_key, 6)
    part_keys = jax.random.split(jax.random.fold_in(root_key, part), 4)
    w_scale = HIDDEN ** -0.5
    seq_shape = (SEQ_LEN, GROUP_BATCH, HIDDEN)
    state_shape = (2, GROUP_BATCH, HIDDEN)

    def weight(w_key):
        return (jax.random.normal(w_key, (HIDDEN, 4 * HIDDEN), jnp.float32) * w_scale).astype(jnp.bfloat16)

    return {
        'seq_in': jax.random.normal(part_keys[0], seq_shape, jnp.float32).astype(jnp.bfloat16),
        'w_x1': weight(shared_keys[0]),
        'w_h1': weight(shared_keys[1]),
        'w_x2': weight(shared_keys[2]),
        'w_h2': weight(shared_keys[3]),
        'bias_1': 0.5 * jax.random.normal(shared_keys[4], (4 * HIDDEN,), jnp.float32),
        'bias_2': 0.5 * jax.random.normal(shared_keys[5], (4 * HIDDEN,), jnp.float32),
        'h_init': 0.6 * jnp.tanh(jax.random.normal(part_keys[1], state_shape, jnp.float32)),
        'c_init': jax.random.normal(part_keys[2], state_shape, jnp.float32),
        'g_out': jax.random.normal(part_keys[3], seq_shape, jnp.float32).astype(jnp.bfloat16),
    }


def gate_acts(pre_act):
    grouped = pre_act.reshape(pre_act.shape[:-1] + (pre_act.shape[-1] // 4, 4))
    squashed = jax.nn.sigmoid(grouped)
    return jnp.stack([squashed[..., 0], squashed[..., 1], jnp.tanh(grouped[..., 2]), squashed[..., 3]], axis=-1)


def cell_grad(dh_tot, dc_next, gate_vals, c_prev, tanh_c):
    in_g = gate_vals[..., 0]
    fgt_g = gate_vals[..., 1]
    cand_g = gate_vals[..., 2]
    out_g = gate_vals[..., 3]
    dc_tot = dc_next + dh_tot * out_g * (1.0 - tanh_c * tanh_c)
    stacked = jnp.stack([
        dc_tot * cand_g * in_g * (1.0 - in_g),
        dc_tot * c_prev * fgt_g * (1.0 - fgt_g),
        dc_tot * in_g * (1.0 - cand_g * cand_g),
        dh_tot * tanh_c * out_g * (1.0 - out_g)], axis=-1)
    return stacked.reshape(stacked.shape[:-2] + (4 * stacked.shape[-2],)), dc_tot * fgt_g


def layer_forward(in_seq, w_in, w_rec, bias_vec, h_start, c_start):
    n_steps, n_batch, in_width = in_seq.shape
    projected = jnp.dot(in_seq.reshape(n_steps * n_batch, in_width), w_in, preferred_element_type=jnp.float32)
    projected = projected.reshape(n_steps, n_batch, w_in.shape[1]) + bias_vec

    def step_fn(carried, u_t):
        h_prev, c_prev = carried
        gate_vals = gate_acts(u_t + jnp.dot(h_prev, w_rec, preferred_element_type=jnp.float32))
        c_new = gate_vals[..., 1] * c_prev + gate_vals[..., 0] * gate_vals[..., 2]
        tanh_c = jnp.tanh(c_new)
        h_new = (gate_vals[..., 3] * tanh_c).astype(jnp.bfloat16)
        return (h_new, c_new), (h_new, c_prev, tanh_c, gate_vals)

    return lax.scan(step_fn, (h_start.astype(jnp.bfloat16), c_start), projected)[1]


def layer_backward(dh_seq, gate_seq, c_prev_seq, tanh_seq, w_rec):
    n_batch = dh_seq.shape[1]
    hid_width = dh_seq.shape[2]

    def step_fn(carried, inputs_t):
        dh_next, dc_next, bias_acc = carried
        dh_out, gate_vals, c_prev, tanh_c = inputs_t
        d_pre, dc_prev = cell_grad(dh_out + dh_next, dc_next, gate_vals, c_prev, tanh_c)
        d_pre_bf = d_pre.astype(jnp.bfloat16)
        dh_rec = lax.dot_general(d_pre_bf, w_rec, (((1,), (1,)), ((), ())), preferred_element_type=jnp.float32)
        return (dh_rec, dc_prev, bias_acc + jnp.sum(d_pre, axis=0)), d_pre_bf

    zero_carry = (jnp.zeros((n_batch, hid_width), jnp.float32), jnp.zeros((n_batch, hid_width), jnp.float32), jnp.zeros((4 * hid_width,), jnp.float32))
    final_carry, dz_seq = lax.scan(step_fn, zero_carry, (dh_seq, gate_seq, c_prev_seq, tanh_seq), reverse=True)
    return dz_seq, final_carry[2]


def seq_contract(left_seq, right_seq):
    n_rows = left_seq.shape[0] * left_seq.shape[1]
    return lax.dot_general(left_seq.reshape(n_rows, left_seq.shape[2]), right_seq.reshape(n_rows, right_seq.shape[2]), (((0,), (0,)), ((), ())), preferred_element_type=jnp.float32)


def reference(seq_in, w_x1, w_h1, w_x2, w_h2, bias_1, bias_2, h_init, c_init, g_out):
    h_first = h_init.astype(jnp.bfloat16)
    h1_seq, c1_prev, tanh_c1, gates_l1 = layer_forward(seq_in, w_x1, w_h1, bias_1, h_init[0], c_init[0])
    h2_seq, c2_prev, tanh_c2, gates_l2 = layer_forward(h1_seq, w_x2, w_h2, bias_2, h_init[1], c_init[1])
    dz_l2, grad_b2 = layer_backward(g_out, gates_l2, c2_prev, tanh_c2, w_h2)
    grad_wh2 = seq_contract(jnp.concatenate([h_first[1:2], h2_seq[:-1]], axis=0), dz_l2)
    grad_wx2 = seq_contract(h1_seq, dz_l2)
    n_steps, n_batch, hid_width = seq_in.shape
    dh_l1 = lax.dot_general(dz_l2.reshape(n_steps * n_batch, 4 * hid_width), w_x2, (((1,), (1,)), ((), ())), preferred_element_type=jnp.float32).reshape(n_steps, n_batch, hid_width)
    dz_l1, grad_b1 = layer_backward(dh_l1, gates_l1, c1_prev, tanh_c1, w_h1)
    grad_wh1 = seq_contract(jnp.concatenate([h_first[0:1], h1_seq[:-1]], axis=0), dz_l1)
    grad_wx1 = seq_contract(seq_in, dz_l1)
    return (grad_wx1, grad_wh1, grad_wx2, grad_wh2, grad_b1, grad_b2)
```

```python
import functools

import jax
import jax.numpy as jnp
from jax import lax
from jax.experimental import pallas as pl
from jax.experimental.pallas import tpu as pltpu
from jax.sharding import PartitionSpec as P

MESH = pl.DeviceIdType.MESH
F32 = jnp.float32
BF16 = jnp.bfloat16
LANE = 128
WIN = 512


def dot(a, b):
    return jnp.dot(a, b, preferred_element_type=F32)


def dot_t(a, b):
    return lax.dot_general(a, b, (((1,), (1,)), ((), ())), preferred_element_type=F32)


def lane_iota(rows):
    return lax.broadcasted_iota(jnp.int32, (rows, LANE), 1)


def join(get, first, count, unit, rows):
    lane = lane_iota(rows)
    tiles = []
    for q in range(-(-count * unit // LANE)):
        lo = q * LANE
        val = get(first + lo // unit)
        for d in range(lo // unit + 1, min((lo + LANE - 1) // unit + 1, count)):
            val = jnp.where(lane >= unit * d - lo, get(first + d), val)
        tiles.append(val)
    return jnp.concatenate(tiles, axis=1)


def split_gates(z, unit):
    lane = lane_iota(z.shape[0])
    tiles = [z[:, q * LANE:(q + 1) * LANE] for q in range(z.shape[1] // LANE)]
    out = []
    for k in range(4):
        q, s = divmod(k * unit, LANE)
        a = tiles[q]
        if s == 0:
            out.append(a)
            continue
        a = pltpu.roll(a, LANE - s, 1)
        if s + unit > LANE:
            a = jnp.where(lane < LANE - s, a, pltpu.roll(tiles[q + 1], LANE - s, 1))
        out.append(a)
    return out


def pack_gates(parts, unit, n_tiles):
    rows = parts[0].shape[0]
    lane = lane_iota(rows)
    rolled = [p if (k * unit) % LANE == 0 else pltpu.roll(p, (k * unit) % LANE, 1) for k, p in enumerate(parts)]
    tiles = []
    for q in range(n_tiles):
        lo = q * LANE
        val = jnp.zeros_like(parts[0])
        for k in range(4):
            a, b = k * unit - lo, (k + 1) * unit - lo
            if b <= 0 or a >= LANE:
                continue
            keep = (lane >= a) & (lane < b)
            val = jnp.where(keep, rolled[k], val)
        tiles.append(val)
    return jnp.concatenate(tiles, axis=1)


def recur_kernel(C, R, T, B, U,
                 x_ref, wx1, wh1, wx2, wh2, bias_ref, h0_ref, c0_ref, g_ref,
                 left_ref, dzn_ref, gb_ref,
                 pm, stage, wf, wt, xs, xr, u1, hist1, hist2, sv, c_in, cst, part, r1, r2, s1, s2,
                 dza, dzacc, gbacc, gbbuf, pxs, zscr, dcs,
                 ws, wr, xss, xrs, css, crs, h1s, h1r, h2s, h2r, b1s, b1r, b2s, b2r, dzs, dzr, gbs, gbr):
    N = C * R
    unit = U // N
    rows = U // R
    cols = 4 * U // C
    ncol = 4 * unit
    npad = stage.shape[-1]
    c = lax.axis_index('col')
    r = lax.axis_index('row')
    me = c * R + r
    my_s = lax.rem(me * unit, LANE)

    def dev(p):
        return {'col': p // R, 'row': lax.rem(p, R)}

    bar = pltpu.get_barrier_semaphore()
    for k in range(1, N):
        pl.semaphore_signal(bar, inc=1, device_id=dev(lax.rem(me + k, N)), device_id_type=MESH)

    def start(src, dst, ss, rs, did):
        pltpu.make_async_remote_copy(src_ref=src, dst_ref=dst, send_sem=ss, recv_sem=rs, device_id=did, device_id_type=MESH).start()

    def wait(ref, sem):
        pltpu.make_async_copy(ref, ref, sem).wait()

    def win(p):
        return pl.multiple_of(jnp.minimum((p * ncol) // LANE * LANE, cols - WIN), LANE)

    kk = lax.broadcasted_iota(jnp.int32, (WIN, npad), 0)
    nn = lax.broadcasted_iota(jnp.int32, (WIN, npad), 1)
    gate = (nn >= unit).astype(jnp.int32) + (nn >= 2 * unit).astype(jnp.int32) + (nn >= 3 * unit).astype(jnp.int32)
    target = jnp.where(nn < ncol, 4 * (nn - unit * gate) + gate, -cols) - kk

    def regroup(w, slot, k):
        p = lax.rem(r + k, R)
        return dot(w[:, pl.ds(win(p), WIN)], pm[p]).astype(BF16)

    my_rows = pl.ds(pl.multiple_of(r * rows, 16), rows)

    def make_pm(k, _):
        p = lax.rem(r + k, R)
        pm[p] = jnp.where(target == win(p) - p * ncol, 1.0, 0.0).astype(BF16)
        stage[0, p] = regroup(wh1, 0, k)
        return 0

    lax.fori_loop(0, R, make_pm, 0)
    pl.semaphore_wait(bar, N - 1)

    def send_w(w):
        def body(k, _):
            p = lax.rem(r + k, R)
            start(stage.at[w, p], wf.at[w, my_rows], ws.at[w], wr.at[w], {'col': c, 'row': p})
            return 0
        lax.fori_loop(1, R, body, 0)
        wf[w, my_rows] = stage[w, r]

    send_w(0)

    owner = r * (N // R) + c

    @pl.when(owner != me)
    def _():
        start(c0_ref, c_in, css, crs, dev(owner))

    @pl.when(owner == me)
    def _():
        c_in[...] = c0_ref[...]

    def xproj(k, _):
        p = lax.rem(r + k, R)
        stage[1, p] = regroup(wh2, 1, k)
        xs[p, pl.ds(0, T * B)] = dot(x_ref[...], regroup(wx1, 0, k))
        xs[p, pl.ds(0, B)] += dot(h0_ref[0], stage[0, p])
        xs[p, pl.ds(T * B, B)] = dot(h0_ref[1], stage[1, p])

        @pl.when(k > 0)
        def _():
            start(xs.at[p], xr.at[r], xss, xrs, {'col': c, 'row': p})
        return 0

    lax.fori_loop(0, R, xproj, 0)
    xr[r] = xs[r]
    send_w(1)

    def third(k, _):
        p = lax.rem(r + k, R)
        stage[2, p] = regroup(wx2, 2, k)
        return 0

    lax.fori_loop(0, R, third, 0)
    send_w(2)

    def wait_w(w):
        wait(stage.at[w, pl.ds(0, R - 1)], wr.at[w])

    wait(xr.at[pl.ds(0, R - 1)], xrs)
    acc = xr[0]
    for k in range(1, R):
        acc = acc + xr[k]
    u1[...] = acc.reshape(T + 1, B, npad)

    @pl.when(owner != me)
    def _():
        wait(c_in, crs)
    cst[...] = c_in[...]

    def transpose_w(w):
        eye = (lax.broadcasted_iota(jnp.int32, (npad, npad), 0) == lax.broadcasted_iota(jnp.int32, (npad, npad), 1))
        eye = jnp.where(eye, 1.0, 0.0).astype(BF16)

        def body(k, _):
            off = pl.multiple_of(k * 256, 256)
            wt[w, :, pl.ds(off, 256)] = dot_t(eye, wf[w, pl.ds(off, 256)]).astype(BF16)
            return 0
        lax.fori_loop(0, U // 256, body, 0)

    def cell(layer, t, z):
        zi, zf, zg, zo = split_gates(z, unit)
        gi, gf, gg, go = jax.nn.sigmoid(zi), jax.nn.sigmoid(zf), jnp.tanh(zg), jax.nn.sigmoid(zo)
        c_prev = cst[layer]
        c_new = gf * c_prev + gi * gg
        tc = jnp.tanh(c_new)
        cst[layer] = c_new
        for k, v in enumerate((gi, gf, gg, go, c_prev, tc)):
            sv[layer, t, k] = v
        return pltpu.roll(go * tc, my_s, 1).astype(BF16)

    def bcast(hist, t, ss, rs):
        for k in range(1, N):
            start(hist.at[t, me], hist.at[t, me], ss.at[t], rs.at[t], dev(lax.rem(me + k, N)))

    def gathered(hist, t):
        return join(lambda d: hist[t, d].astype(F32), 0, N, unit, B).astype(BF16)

    hist1[0, me] = cell(0, 0, u1[0] + bias_ref[0])
    bcast(hist1, 0, h1s, h1r)
    wait_w(0)
    wait_w(1)
    wait_w(2)

    def fwd(s, _):
        wait(hist1.at[s, pl.ds(0, N - 1)], h1r.at[s])
        h_full = gathered(hist1, s)

        @pl.when(s < T - 1)
        def _():
            hist1[s + 1, me] = cell(0, s + 1, u1[s + 1] + bias_ref[0] + dot(h_full, wf[0]))
            bcast(hist1, s + 1, h1s, h1r)

        zx = dot(h_full, wf[2]) + bias_ref[1]

        @pl.when(s == 0)
        def _():
            zscr[...] = u1[T]

        @pl.when(s > 0)
        def _():
            wait(hist2.at[s - 1, pl.ds(0, N - 1)], h2r.at[s - 1])
            zscr[...] = dot(gathered(hist2, s - 1), wf[1])

        hist2[s, me] = cell(1, s, zx + zscr[...])

        @pl.when(s < T - 1)
        def _():
            bcast(hist2, s, h2s, h2r)

        for w in range(3):
            @pl.when(s == w + 2)
            def _():
                transpose_w(w)
        return 0

    lax.fori_loop(0, T, fwd, 0)

    gbacc[...] = jnp.zeros_like(gbacc)
    dcs[...] = jnp.zeros_like(dcs)

    def cell_grad(layer, t, dh):
        gi, gf, gg, go, c_prev, tc = [sv[layer, t, k] for k in range(6)]
        dc = dcs[layer] + dh * go * (1.0 - tc * tc)
        dz = (dc * gg * gi * (1.0 - gi), dc * c_prev * gf * (1.0 - gf), dc * gi * (1.0 - gg * gg), dh * tc * go * (1.0 - go))
        dcs[layer] = dc * gf
        for k in range(4):
            gbacc[layer, k] += dz[k]
        packed = pack_gates(dz, unit, npad // LANE).astype(BF16)
        dza[layer, r, t] = packed
        return packed

    lane_b = lane_iota(B)

    def scatter(p, sbuf, rbuf, t, ss, rs):
        tiles = [p[:, q * LANE:(q + 1) * LANE] for q in range(U // LANE)]
        for d in range(N):
            q, s = divmod(d * unit, LANE)
            v = tiles[q]
            if s + unit > LANE:
                v = jnp.where(lane_b >= s, v, tiles[q + 1])
            sbuf[t, d] = v
        for k in range(1, N):
            d = lax.rem(me + k, N)
            start(sbuf.at[t, d], rbuf.at[t, me], ss.at[t], rs.at[t], dev(d))
        rbuf[t, me] = sbuf[t, me]

    def reduced(rbuf, t, rs):
        wait(rbuf.at[t, pl.ds(0, N - 1)], rs.at[t])
        vals = [rbuf[t, d] for d in range(N)]
        while len(vals) > 1:
            vals = [a + b for a, b in zip(vals[::2], vals[1::2])]
        return pltpu.roll(vals[0], lax.rem(LANE - my_s, LANE), 1)

    CH = 4

    def send_dz(layer, t):
        @pl.when(lax.rem(t, CH) == 0)
        def _():
            ts = pl.ds(t, CH)
            for k in range(1, R):
                start(dza.at[layer, r, ts], dza.at[layer, r, ts], dzs.at[layer, t // CH], dzr.at[layer, t // CH],
                      {'col': c, 'row': lax.rem(r + k, R)})

    def bwd(s, _):
        t = T - 1 - s
        part[...] = g_ref[t].astype(F32)

        @pl.when(s > 0)
        def _():
            part[...] += reduced(r2, t, b2r)

        dz2 = cell_grad(1, t, part[...])

        @pl.when(t > 0)
        def _():
            scatter(dot(dz2, wt[1]), s2, r2, t - 1, b2s, b2r)

        pxs[...] = dot(dz2, wt[2])
        send_dz(1, t)

        @pl.when(s > 0)
        def _():
            dz1 = cell_grad(0, t + 1, reduced(r1, t + 1, b1r))
            pxs[...] += dot(dz1, wt[0])

        scatter(pxs[...], s1, r1, t, b1s, b1r)

        @pl.when(s > 0)
        def _():
            send_dz(0, t + 1)
        return 0

    lax.fori_loop(0, T, bwd, 0)
    cell_grad(0, 0, reduced(r1, 0, b1r))
    send_dz(0, 0)

    sub = lax.broadcasted_iota(jnp.int32, (8, LANE), 0)
    packed = []
    for k in range(4):
        b0 = jnp.sum(gbacc[0, k], axis=0, keepdims=True)
        b1 = jnp.sum(gbacc[1, k], axis=0, keepdims=True)
        packed.append(jnp.where(sub == 0, jnp.broadcast_to(b0, (8, LANE)), jnp.broadcast_to(b1, (8, LANE))))
    gbbuf[r] = pack_gates(packed, unit, npad // LANE)
    for k in range(1, R):
        start(gbbuf.at[r], gbbuf.at[r], gbs, gbr, {'col': c, 'row': lax.rem(r + k, R)})

    shift = lax.rem(LANE * rows - r * rows, LANE)
    per = N // R

    def local_rows(hist, count):
        def get(d):
            v = hist[pl.ds(0, count), per * r + d].astype(F32).reshape(count * B, LANE)
            return pltpu.roll(v, shift, 1)
        return join(get, 0, per, unit, count * B)

    h1_rows = local_rows(hist1, T)
    h2_rows = local_rows(hist2, T - 1)

    def h0_rows(layer):
        return jnp.concatenate([h0_ref[layer].astype(F32), jnp.zeros((B, npad - rows), F32)], axis=1)

    left_ref[0] = jnp.concatenate([h0_rows(0), h1_rows[:(T - 1) * B]], axis=0).astype(BF16)
    left_ref[1] = h1_rows.astype(BF16)
    left_ref[2] = jnp.concatenate([h0_rows(1), h2_rows], axis=0).astype(BF16)

    for layer in (1, 0):
        for q in range(T // CH):
            wait(dza.at[layer, pl.ds(0, R - 1), pl.ds(0, CH)], dzr.at[layer, q])
        dzacc[...] = jnp.zeros_like(dzacc)
        for p in range(R):
            st = min(p * ncol // LANE * LANE, cols - WIN)
            dzp = dza[layer, p].astype(F32).reshape(T * B, npad).astype(BF16)
            dzacc[:, st:st + WIN] += dot_t(dzp, pm[p])
        dzn_ref[layer] = dzacc[...].astype(BF16)
    wait(gbbuf.at[pl.ds(0, R - 1)], gbr)
    gb_ref[...] = gbbuf[...]

    for w in range(3):
        wait(stage.at[w, pl.ds(0, R - 1)], ws.at[w])
    wait(xs.at[pl.ds(0, R - 1)], xss)

    @pl.when(owner != me)
    def _():
        wait(c_in, css)

    def drain(t, _):
        wait(hist1.at[t, pl.ds(0, N - 1)], h1s.at[t])
        wait(s1.at[t, pl.ds(0, N - 1)], b1s.at[t])

        @pl.when(t < T - 1)
        def _():
            wait(hist2.at[t, pl.ds(0, N - 1)], h2s.at[t])
            wait(s2.at[t, pl.ds(0, N - 1)], b2s.at[t])
        return 0

    lax.fori_loop(0, T, drain, 0)
    for layer in range(2):
        for q in range(T // CH):
            wait(dza.at[layer, pl.ds(0, R - 1), pl.ds(0, CH)], dzs.at[layer, q])
    wait(gbbuf.at[pl.ds(0, R - 1)], gbs)


def grad_kernel(x_ref, left_ref, dzn_ref, gx1, gh1, gx2, gh2):
    rows = gx1.shape[0]
    tn = (((0,), (0,)), ((), ()))

    def mm(a, b):
        return lax.dot_general(a, b, tn, preferred_element_type=F32)

    gx1[...] = mm(x_ref[...], dzn_ref[0])
    gh1[...] = mm(left_ref[0], dzn_ref[0])[:rows]
    gx2[...] = mm(left_ref[1], dzn_ref[1])[:rows]
    gh2[...] = mm(left_ref[2], dzn_ref[1])[:rows]


def solution(mesh):
    C, R = mesh.shape['col'], mesh.shape['row']
    N = C * R
    seq_spec = P(None, 'data', 'row')
    w_spec = P('row', 'col')
    bias_spec = P('col')
    g_spec = P(None, 'data', 'col')
    grad_spec = P(('data', 'row'), 'col')
    gbias_spec = P(('data', 'col'))

    def local_grads(seq_in, w_x1, w_h1, w_x2, w_h2, bias_1, bias_2, h_init, c_init, g_out):
        T, B, rows = seq_in.shape
        U = rows * R
        cols = w_x1.shape[1]
        unit = U // N
        ncol = 4 * unit
        nt = -(-ncol // LANE)
        npad = nt * LANE
        r = lax.axis_index('row')
        c = lax.axis_index('col')

        x2d = seq_in.reshape(T * B, rows)
        h0 = h_init.astype(BF16)
        c0 = jnp.pad(lax.dynamic_slice_in_dim(c_init, c * unit, unit, axis=2), ((0, 0), (0, 0), (0, LANE - unit)))
        g = jnp.pad(lax.dynamic_slice_in_dim(g_out, r * unit, unit, axis=2), ((0, 0), (0, 0), (0, LANE - unit)))
        bias = lax.dynamic_slice_in_dim(jnp.stack([bias_1, bias_2]), r * ncol, ncol, axis=1)
        bias = jnp.swapaxes(bias.reshape(2, unit, 4), 1, 2).reshape(2, 1, ncol)
        bias = jnp.broadcast_to(jnp.pad(bias, ((0, 0), (0, 0), (0, npad - ncol))), (2, B, npad))

        vm = pl.BlockSpec(memory_space=pltpu.VMEM)
        dma = pltpu.SemaphoreType.DMA
        V = pltpu.VMEM
        left, dzn, gb = pl.pallas_call(
            functools.partial(recur_kernel, C, R, T, B, U),
            name='recur',
            out_shape=(jax.ShapeDtypeStruct((3, T * B, npad), BF16), jax.ShapeDtypeStruct((2, T * B, cols), BF16),
                       jax.ShapeDtypeStruct((R, 8, npad), F32)),
            in_specs=[vm] * 9,
            out_specs=(vm, vm, vm),
            scratch_shapes=[
                V((R, WIN, npad), BF16),
                V((3, R, rows, npad), BF16),
                V((3, U, npad), BF16),
                V((3, npad, U), BF16),
                V((R, (T + 1) * B, npad), F32),
                V((R, (T + 1) * B, npad), F32),
                V((T + 1, B, npad), F32),
                V((T, N, B, LANE), BF16),
                V((T, N, B, LANE), BF16),
                V((2, T, 6, B, LANE), F32),
                V((2, B, LANE), F32),
                V((2, B, LANE), F32),
                V((B, LANE), F32),
                V((T, N, B, LANE), F32),
                V((T, N, B, LANE), F32),
                V((T, N, B, LANE), F32),
                V((T, N, B, LANE), F32),
                V((2, R, T, B, npad), BF16),
                V((T * B, cols), F32),
                V((2, 4, B, LANE), F32),
                V((R, 8, npad), F32),
                V((B, U), F32),
                V((B, npad), F32),
                V((2, B, LANE), F32),
                dma((3,)), dma((3,)), dma, dma, dma, dma,
                dma((T,)), dma((T,)), dma((T,)), dma((T,)),
                dma((T,)), dma((T,)), dma((T,)), dma((T,)),
                dma((2, T // 4)), dma((2, T // 4)), dma, dma,
            ],
            compiler_params=pltpu.CompilerParams(collective_id=0, has_side_effects=True, vmem_limit_bytes=62 * 1024 * 1024),
        )(x2d, w_x1, w_h1, w_x2, w_h2, bias, h0, c0, g)

        tn = 256
        out = jax.ShapeDtypeStruct((rows, cols), F32)
        ospec = pl.BlockSpec((rows, tn), lambda i: (0, i))
        grads = pl.pallas_call(
            grad_kernel,
            name='grads',
            grid=(cols // tn,),
            out_shape=(out,) * 4,
            in_specs=[pl.BlockSpec((T * B, rows), lambda i: (0, 0)), pl.BlockSpec((3, T * B, npad), lambda i: (0, 0, 0)),
                      pl.BlockSpec((2, T * B, tn), lambda i: (0, 0, i))],
            out_specs=(ospec,) * 4,
        )(x2d, left, dzn)
        gbt = jnp.swapaxes(gb[:, :2, :ncol].reshape(R, 2, 4, unit), 2, 3)
        gb1 = gbt[:, 0].reshape(cols)
        gb2 = gbt[:, 1].reshape(cols)
        return (*grads, gb1, gb2)

    return jax.shard_map(local_grads, mesh=mesh,
                         in_specs=(seq_spec, w_spec, w_spec, w_spec, w_spec, bias_spec, bias_spec, seq_spec, seq_spec, g_spec),
                         out_specs=(grad_spec, grad_spec, grad_spec, grad_spec, gbias_spec, gbias_spec),
                         check_vma=False)
```

```python
import functools

import jax
import jax.numpy as jnp
from jax import lax
from jax.experimental import pallas as pl
from jax.experimental.pallas import tpu as pltpu
from jax.sharding import PartitionSpec as P

MESH = pl.DeviceIdType.MESH
F32 = jnp.float32
BF16 = jnp.bfloat16
LANE = 128
WIN = 512
CH = 4
X_CUTS = (0, 6, 9, 12, 16)
X_SEND = (None, 2, 4, 6)
W2_CUTS = (0, 128, 240, 352)
GROWS = 4
WROWS = 32


def dot(a, b):
    return jnp.dot(a, b, preferred_element_type=F32)


def dot_t(a, b):
    return lax.dot_general(a, b, (((1,), (1,)), ((), ())), preferred_element_type=F32)


def by_thirds(x, f):
    x = x * 0.25
    hi = x.astype(BF16)
    rest = x - hi.astype(F32)
    mid = rest.astype(BF16)
    lo = (rest - mid.astype(F32)).astype(BF16)
    return ((f(hi) + f(mid)) + f(lo)) * 4.0


def lane_iota(rows):
    return lax.broadcasted_iota(jnp.int32, (rows, LANE), 1)


def join(segs, width):
    lane = lane_iota(segs[0][1].shape[0])
    tiles = []
    for lo in range(0, width, LANE):
        val = None
        for i, (start, tile) in enumerate(segs):
            end = segs[i + 1][0] if i + 1 < len(segs) else width
            if end <= lo or start >= lo + LANE:
                continue
            val = tile if val is None else jnp.where(lane >= start - lo, tile, val)
        tiles.append(val)
    return jnp.concatenate(tiles, axis=1)


def split_gates(z, unit):
    lane = lane_iota(z.shape[0])
    tiles = [z[:, q * LANE:(q + 1) * LANE] for q in range(z.shape[1] // LANE)]
    out = []
    for k in range(4):
        q, s = divmod(k * unit, LANE)
        a = tiles[q]
        if s:
            a = pltpu.roll(a, LANE - s, 1)
            if s + unit > LANE:
                a = jnp.where(lane < LANE - s, a, pltpu.roll(tiles[q + 1], LANE - s, 1))
        out.append(a)
    return out


def pack_gates(parts, unit, n_tiles):
    lane = lane_iota(parts[0].shape[0])
    rolled = [p if (k * unit) % LANE == 0 else pltpu.roll(p, (k * unit) % LANE, 1) for k, p in enumerate(parts)]
    tiles = []
    for q in range(n_tiles):
        val = jnp.zeros_like(parts[0])
        for k in range(4):
            a, b = k * unit - q * LANE, (k + 1) * unit - q * LANE
            if b > 0 and a < LANE:
                val = jnp.where((lane >= a) & (lane < b), rolled[k], val)
        tiles.append(val)
    return jnp.concatenate(tiles, axis=1)


def recur_kernel(C, R, T, B, U,
                 x_ref, wx1_ref, wh1_ref, wx2_ref, wh2_ref, b1_ref, b2_ref, hi_ref, ci_ref, g_ref,
                 left_ref, dzn_ref, gb_ref,
                 wx1, wh1, wx2, wh2, brow, pm, stage, xstage, wf, wt, wc1, wc2, xsib, xs, xr, zs, zr, h0, hist1, hist2, sv, c_out, c_in, cst,
                 bias, gs, part, r1, r2, s1, s2, dzo, dza, gbacc, gbbuf, pxs, zscr, dcs, d1, hspare, ins,
                 ws, wr, sbs, sbr, xss, xrs, zss, zrs, h0s, h0r, css, crs, h1s, h1r, h2s, h2r,
                 b1s, b1r, b2s, b2r, dzs, dzr, gbs, gbr):
    N = C * R
    CHIPS = R // 2
    unit = U // N
    rows = U // R
    cols = 4 * U // C
    ncol = 4 * unit
    npad = stage.shape[-1]
    c = lax.axis_index('col')
    r = lax.axis_index('row')
    me = c * R + r
    chip, core = r // 2, lax.rem(r, 2)
    sib = {'col': c, 'row': chip * 2 + 1 - core}
    my_s = lax.rem(r * unit, LANE)
    group = unit * R
    gw = -(-group // LANE) * LANE
    ring = lambda o, n: min(o, n - o)
    far_y = sorted(range(C), key=lambda o: -ring(o, C))
    far_row = sorted(((dx, dk) for dx in range(CHIPS) for dk in range(2)), key=lambda o: -ring(o[0], CHIPS))

    def col_at(dy):
        return lax.rem(c + dy, C)

    def row_at(dx, dk):
        return 2 * lax.rem(chip + dx, CHIPS) + lax.rem(core + dk, 2)

    peers = [(dy, dx, dk) for dy in range(C) for dx, dk in far_row if (dy, dx, dk) != (0, 0, 0)]
    peers.sort(key=lambda o: -(ring(o[0], C) + ring(o[1], CHIPS)))

    loads = [pltpu.make_async_copy(a, b, ins.at[i]) for i, (a, b) in
             enumerate(((wh1_ref, wh1), (wx1_ref, wx1), (wh2_ref, wh2), (wx2_ref, wx2)))]
    for load in loads:
        load.start()

    def dev(p):
        return {'col': p // R, 'row': lax.rem(p, R)}

    def row_dev(p):
        return {'col': c, 'row': p}

    bar = pltpu.get_barrier_semaphore()
    for k in range(1, N):
        pl.semaphore_signal(bar, inc=1, device_id=dev(lax.rem(me + k, N)), device_id_type=MESH)

    def start(src, dst, ss, rs, did):
        pltpu.make_async_remote_copy(src_ref=src, dst_ref=dst, send_sem=ss, recv_sem=rs, device_id=did, device_id_type=MESH).start()

    def wait(ref, sem):
        pltpu.make_async_copy(ref, ref, sem).wait()

    def win(p):
        return pl.multiple_of(jnp.minimum((p * ncol) // LANE * LANE, cols - WIN), LANE)

    kk = lax.broadcasted_iota(jnp.int32, (WIN, npad), 0)
    nn = lax.broadcasted_iota(jnp.int32, (WIN, npad), 1)
    gate = (nn >= unit).astype(jnp.int32) + (nn >= 2 * unit).astype(jnp.int32) + (nn >= 3 * unit).astype(jnp.int32)
    target = jnp.where(nn < ncol, 4 * (nn - unit * gate) + gate, -cols) - kk

    def regroup(w, p):
        return dot(w[:, pl.ds(win(p), WIN)], pm[p]).astype(BF16)

    def row_block(p):
        return pl.ds(pl.multiple_of(p * rows, 16), rows)

    def make_pm(p, _):
        pm[p] = jnp.where(target == win(p) - p * ncol, 1.0, 0.0).astype(BF16)
        return 0

    h0[r] = jnp.concatenate([hi_ref[...], jnp.zeros((2, B, npad - rows), F32)], axis=2).astype(BF16)
    lax.fori_loop(0, R, make_pm, 0)
    pl.semaphore_wait(bar, N - 1)
    start(x_ref, xsib, sbs.at[0], sbr.at[0], sib)
    for dx, dk in far_row:
        if (dx, dk) != (0, 0):
            start(h0.at[r], h0.at[r], h0s, h0r, row_dev(row_at(dx, dk)))
    loads[0].wait()

    def send_h1(k, _):
        p = lax.rem(r + R // 2 + k, R)
        stage[0, p] = regroup(wh1, p)

        @pl.when(p != r)
        def _():
            start(stage.at[0, p], wf.at[0, row_block(r)], ws.at[0], wr.at[0], row_dev(p))
        return 0

    lax.fori_loop(0, R, send_h1, 0)
    wf[0, row_block(r)] = stage[0, r]

    def send_h2(cut):
        lo, hi = W2_CUTS[cut], W2_CUTS[cut + 1]
        for dx, dk in far_row:
            if (dx, dk) != (0, 0):
                p = row_at(dx, dk)
                start(stage.at[1, p, pl.ds(lo, hi - lo)], wf.at[1, pl.ds(pl.multiple_of(r * rows + lo, 16), hi - lo)],
                      ws.at[1], wr.at[1], row_dev(p))

    owner = r * (N // R) + c
    ci = jnp.concatenate([ci_ref[...].reshape(2 * B, rows), jnp.zeros((2 * B, npad - rows), F32)], axis=1)
    lane2 = lane_iota(2 * B)
    for j in range(C):
        q, s = divmod(j * unit, LANE)
        v = ci[:, q * LANE:(q + 1) * LANE]
        if s:
            v = pltpu.roll(v, LANE - s, 1)
            if s + unit > LANE:
                v = jnp.where(lane2 < LANE - s, v, pltpu.roll(ci[:, (q + 1) * LANE:(q + 2) * LANE], LANE - s, 1))
        v = jnp.where(lane2 < unit, v, 0.0).reshape(2, B, LANE)

        @pl.when(c == j)
        def _():
            c_out[...] = v

    @pl.when(owner != me)
    def _():
        start(c_out, c_in, css, crs, dev(owner))

    @pl.when(owner == me)
    def _():
        c_in[...] = c_out[...]

    def trade1(j, _):
        mine, other = 2 * j + core, 2 * j + 1 - core
        wc1[j, row_block(core)] = regroup(wx1, mine)
        xstage[j] = regroup(wx1, other)
        start(xstage.at[j], wc1.at[j, row_block(core)], sbs.at[1], sbr.at[1], sib)
        return 0

    loads[1].wait()
    lax.fori_loop(0, CHIPS, trade1, 0)
    loads[2].wait()

    def stage_h2(p, _):
        stage[1, p] = regroup(wh2, p)
        return 0

    lax.fori_loop(0, R, stage_h2, 0)
    wait(xsib, sbr.at[0])
    wait(xstage, sbr.at[1])

    def flat(v):
        return v.astype(F32).reshape(T * B, rows).astype(BF16)

    def xproj(j, _):
        v = dot(flat(x_ref[...]), wc1[j, row_block(core)]) + dot(flat(xsib[...]), wc1[j, row_block(1 - core)])
        xs[j] = v.reshape(T, B, npad)
        return 0

    lax.fori_loop(0, CHIPS, xproj, 0)

    def send_x(cut):
        ts = pl.ds(X_CUTS[cut], X_CUTS[cut + 1] - X_CUTS[cut])
        for k in (2, 1, 3):
            j = lax.rem(chip + k, CHIPS)
            start(xs.at[j, ts], xr.at[chip, ts], xss.at[cut], xrs.at[cut], row_dev(2 * j + core))

    def wait_x(cut, sems):
        wait(xs.at[pl.ds(0, CHIPS - 1), pl.ds(X_CUTS[cut], X_CUTS[cut + 1] - X_CUTS[cut])], sems.at[cut])

    send_x(0)
    xr[chip] = xs[chip]
    send_h2(0)
    wf[1, row_block(r)] = stage[1, r]
    loads[3].wait()

    def trade2(j, _):
        mine, other = 2 * j + core, 2 * j + 1 - core
        blk = regroup(wx2, mine)
        stage[2, mine] = blk
        wc2[j, row_block(core)] = blk
        stage[2, other] = regroup(wx2, other)
        start(stage.at[2, other], wc2.at[j, row_block(core)], sbs.at[2], sbr.at[2], sib)
        return 0

    lax.fori_loop(0, CHIPS, trade2, 0)
    wf[2, row_block(r)] = stage[2, r]

    for l, ref in enumerate((b1_ref, b2_ref)):
        brow[...] = jnp.broadcast_to(ref[...].reshape(1, cols), (B, cols))
        b = brow[:, pl.ds(win(r), WIN)]
        bias[l] = by_thirds(b, lambda v: dot(v, pm[r]))
    g_w = g_ref.shape[2]
    sel_k = lax.broadcasted_iota(jnp.int32, (g_w, LANE), 0)
    sel_n = lax.broadcasted_iota(jnp.int32, (g_w, LANE), 1)
    sel = jnp.where((sel_k == sel_n + r * unit) & (sel_n < unit), 1.0, 0.0).astype(BF16)
    gs[...] = dot(g_ref[...].astype(F32).reshape(T * B, g_w).astype(BF16), sel).reshape(T, B, LANE)

    def transpose_w(w):
        eye = (lax.broadcasted_iota(jnp.int32, (npad, npad), 0) == lax.broadcasted_iota(jnp.int32, (npad, npad), 1))
        eye = jnp.where(eye, 1.0, 0.0).astype(BF16)

        def body(k, _):
            for off in range(0, group, 256):
                n = min(256, group - off)
                v = dot_t(eye, wf[w, pl.ds(pl.multiple_of(k * group + off, 16), n)]).astype(BF16)
                if off + n == group and gw > group:
                    v = jnp.concatenate([v, jnp.zeros((npad, gw - group), BF16)], axis=1)
                wt[w, :, pl.ds(pl.multiple_of(k * gw + off, LANE), v.shape[1])] = v
            return 0
        lax.fori_loop(0, C, body, 0)

    def cell(layer, t, z):
        zi, zf, zg, zo = split_gates(z, unit)
        gi, gf, gg, go = jax.nn.sigmoid(zi), jax.nn.sigmoid(zf), jnp.tanh(zg), jax.nn.sigmoid(zo)
        c_prev = cst[layer]
        c_new = gf * c_prev + gi * gg
        tc = jnp.tanh(c_new)
        cst[layer] = c_new
        for k, v in enumerate((gi, gf, gg, go, c_prev, tc)):
            sv[layer, t, k] = v
        return pltpu.roll(go * tc, my_s, 1).astype(BF16)

    def bcast(hist, t, ss, rs):
        for dy, dx, dk in peers:
            start(hist.at[t, c, r], hist.at[t, c, r], ss.at[t], rs.at[t, c], {'col': col_at(dy), 'row': row_at(dx, dk)})

    def group_h(hist, t, cs):
        return join([(unit * d, hist[t, cs, d].astype(F32)) for d in range(R)], gw)[:, :group].astype(BF16)

    def h_times(hist, t, rs, w):
        z = jnp.zeros((B, npad), F32)
        for dy in far_y[::-1]:
            cs = col_at(dy)
            wait(hist.at[t, cs, pl.ds(0, R if dy else R - 1)], rs.at[t, cs])
            z = z + dot(group_h(hist, t, cs), wf[w, pl.ds(pl.multiple_of(cs * group, 16), group)])
        return z

    def from_h0(layer):
        v = jnp.zeros((B, npad), F32)
        for p in range(R):
            v = v + dot(h0[p, layer][:, :rows], wf[layer, p * rows:(p + 1) * rows])
        return v

    def total(ref, t):
        return (ref[0, t] + ref[1, t]) + (ref[2, t] + ref[3, t])

    def partial_z2(t):
        h = group_h(hist1, t, chip)
        for j in range(CHIPS):
            zs[j, t] = dot(h, wc2[j])
        for k in (2, 1, 3):
            j = lax.rem(chip + k, CHIPS)
            start(zs.at[j, t], zr.at[chip, t], zss.at[t], zrs.at[t], row_dev(2 * j + core))
        zr[chip, t] = zs[chip, t]

    @pl.when(owner != me)
    def _():
        wait(c_in, crs)
    cst[...] = c_in[...]
    wait(h0.at[pl.ds(0, R - 1)], h0r)
    wait_x(0, xrs)
    wait(stage.at[0, pl.ds(0, R - 1)], wr.at[0])
    hist1[0, c, r] = cell(0, 0, total(xr, 0) + bias[0] + from_h0(0))
    bcast(hist1, 0, h1s, h1r)
    send_h2(1)
    wait(xstage, sbr.at[2])

    n_pieces = rows // WROWS

    def fwd(s, _):
        for cut in range(1, len(X_CUTS) - 1):
            @pl.when(s == X_CUTS[cut] - 1)
            def _():
                wait_x(cut, xrs)

        @pl.when(s < T - 1)
        def _():
            hist1[s + 1, c, r] = cell(0, s + 1, total(xr, s + 1) + bias[0] + h_times(hist1, s, h1r, 0))
            bcast(hist1, s + 1, h1s, h1r)

        @pl.when(s == T - 1)
        def _():
            for dy in range(C):
                cs = col_at(dy)
                wait(hist1.at[s, cs, pl.ds(0, R if dy else R - 1)], h1r.at[s, cs])

        @pl.when(s < T)
        def _():
            partial_z2(s)

        @pl.when(s == 0)
        def _():
            send_h2(2)

        @pl.when(s == 1)
        def _():
            wait(stage.at[1, pl.ds(0, R - 1)], wr.at[1])
            zscr[...] = from_h0(1)

        @pl.when(s > 1)
        def _():
            zscr[...] = h_times(hist2, s - 2, h2r, 1)

        @pl.when(s > 0)
        def _():
            wait(zs.at[pl.ds(0, CHIPS - 1), s - 1], zrs.at[s - 1])
            hist2[s - 1, c, r] = cell(1, s - 1, total(zr, s - 1) + bias[1] + zscr[...])

            @pl.when(s < T)
            def _():
                bcast(hist2, s - 1, h2s, h2r)

        for cut in range(1, len(X_CUTS) - 1):
            @pl.when(s == X_SEND[cut])
            def _():
                send_x(cut)

        @pl.when((s >= 3) & (s < 3 + n_pieces))
        def _():
            piece = pl.ds(pl.multiple_of((s - 3) * WROWS, WROWS), WROWS)
            dest = pl.ds(pl.multiple_of(r * rows + (s - 3) * WROWS, WROWS), WROWS)
            for k in range(1, R):
                p = lax.rem(r + k, R)
                start(stage.at[2, p, piece], wf.at[2, dest], ws.at[2], wr.at[2], row_dev(p))

        @pl.when(s == 2)
        def _():
            transpose_w(0)

        @pl.when(s == 4)
        def _():
            transpose_w(1)

        @pl.when(s == T - 1)
        def _():
            wait(stage.at[2, pl.ds(0, R - 1)], wr.at[2])
            transpose_w(2)
        return 0

    lax.fori_loop(0, T + 1, fwd, 0)

    gbacc[...] = jnp.zeros_like(gbacc)
    dcs[...] = jnp.zeros_like(dcs)

    def cell_grad(layer, t, dh):
        gi, gf, gg, go, c_prev, tc = [sv[layer, t, k] for k in range(6)]
        dc = dcs[layer] + dh * go * (1.0 - tc * tc)
        dz = (dc * gg * gi * (1.0 - gi), dc * c_prev * gf * (1.0 - gf), dc * gi * (1.0 - gg * gg), dh * tc * go * (1.0 - go))
        dcs[layer] = dc * gf
        for k in range(4):
            gbacc[layer, k] += dz[k]
        packed = pack_gates(dz, unit, npad // LANE).astype(BF16)
        dzo[layer, t] = packed
        return packed

    lane_b = lane_iota(B)

    def scatter(term, sbuf, rbuf, t, ss, rs):
        for i, dy in enumerate(far_y):
            cs = col_at(dy)
            p = term(pl.ds(pl.multiple_of(cs * gw, LANE), gw))
            tiles = [p[:, q * LANE:(q + 1) * LANE] for q in range(gw // LANE)]
            for d in range(R):
                q, off = divmod(d * unit, LANE)
                v = tiles[q]
                if off + unit > LANE:
                    v = jnp.where(lane_b >= off, v, tiles[q + 1])
                sbuf[t, i, d] = v
            for dx, dk in far_row:
                if (dy, dx, dk) != (0, 0, 0):
                    p = row_at(dx, dk)
                    start(sbuf.at[t, i, p], rbuf.at[t, me], ss.at[t], rs.at[t], {'col': cs, 'row': p})
            if dy == 0:
                rbuf[t, me] = sbuf[t, i, r]

    def reduced(rbuf, t, rs):
        wait(rbuf.at[t, pl.ds(0, N - 1)], rs.at[t])
        vals = [rbuf[t, d] for d in range(N)]
        while len(vals) > 1:
            vals = [a + b for a, b in zip(vals[::2], vals[1::2])]
        return pltpu.roll(vals[0], lax.rem(LANE - my_s, LANE), 1)

    order = pm.at[0, pl.ds(0, npad)]

    def send_dz(layer, t):
        @pl.when(lax.rem(t, CH) == 0)
        def _():
            ts = pl.ds(t, CH)
            v = dzo[layer, ts].astype(F32).reshape(CH * B, npad).astype(BF16)
            dza[layer, r, ts] = dot_t(v, order[...]).reshape(CH, B, npad).astype(BF16)
            for k in range(1, R):
                start(dza.at[layer, r, ts], dza.at[layer, r, ts], dzs.at[layer, t // CH], dzr.at[layer, t // CH],
                      row_dev(lax.rem(r + k, R)))

    def blocks_joined(get):
        segs = []
        for p in range(R):
            v = get(p)
            for a in range(npad // LANE):
                tile = v[:, a * LANE:(a + 1) * LANE]
                s = (p * ncol) % LANE
                segs.append((p * ncol + a * LANE, pltpu.roll(tile, s, 1) if s else tile))
        return join(segs, cols)

    def place_dz(q):
        for layer in range(2):
            wait(dza.at[layer, pl.ds(0, R - 1), pl.ds(0, CH)], dzr.at[layer, q])
            v = blocks_joined(lambda p: dza[layer, p, pl.ds(q * CH, CH)].astype(F32).reshape(CH * B, npad))
            dzn_ref[layer, pl.ds(pl.multiple_of(q * (CH * B), CH * B), CH * B)] = v.astype(BF16)

    shift = core * ((LANE - rows % LANE) % LANE)
    per = R // 2

    def local_rows(hist, count):
        segs = [(unit * d, pltpu.roll(hist[pl.ds(0, count), chip, per * core + d].astype(F32).reshape(count * B, LANE), shift, 1))
                for d in range(per)]
        return join(segs, npad)

    def put_left(i, v):
        for a in range(npad // LANE):
            left_ref[i, a * LANE:(a + 1) * LANE] = v[:, a * LANE:(a + 1) * LANE].T.astype(BF16)

    def wide(v):
        return jnp.concatenate([v, jnp.zeros((v.shape[0], npad - rows), F32)], axis=1)

    def bwd(s, _):
        t = T - 1 - s
        part[...] = gs[t]

        @pl.when(s > 0)
        def _():
            part[...] += reduced(r2, t, b2r)

        dz2 = cell_grad(1, t, part[...])

        @pl.when(t > 0)
        def _():
            scatter(lambda n: dot(dz2, wt[1, :, n]), s2, r2, t - 1, b2s, b2r)

        pxs[...] = dot(dz2, wt[2])
        send_dz(1, t)

        @pl.when(s == 0)
        def _():
            d1[...] = jnp.zeros_like(d1)

        @pl.when(s > 0)
        def _():
            d1[...] = cell_grad(0, t + 1, reduced(r1, t + 1, b1r))

        scatter(lambda n: dot(d1[...], wt[0, :, n]) + pxs[:, n], s1, r1, t, b1s, b1r)

        @pl.when(s > 0)
        def _():
            send_dz(0, t + 1)

        @pl.when((s >= CH + 2) & (lax.rem(s, CH) == 2))
        def _():
            place_dz(T // CH - 1 - (s - CH - 2) // CH)

        @pl.when(s == 1)
        def _():
            put_left(0, wide(x_ref[...].astype(F32).reshape(T * B, rows)))

        @pl.when(s == 2)
        def _():
            h1_rows = local_rows(hist1, T)
            put_left(2, h1_rows)
            first = h0[r, 0].astype(F32)
            put_left(1, jnp.concatenate([first, h1_rows[:(T - 1) * B]], axis=0))

        @pl.when(s == 3)
        def _():
            put_left(3, jnp.concatenate([h0[r, 1].astype(F32), local_rows(hist2, T - 1)], axis=0))
        return 0

    lax.fori_loop(0, T, bwd, 0)
    cell_grad(0, 0, reduced(r1, 0, b1r))
    send_dz(0, 0)

    sub = lax.broadcasted_iota(jnp.int32, (8, LANE), 0)
    packed = []
    for k in range(4):
        b0 = jnp.sum(gbacc[0, k], axis=0, keepdims=True)
        b1 = jnp.sum(gbacc[1, k], axis=0, keepdims=True)
        packed.append(jnp.where(sub == 0, jnp.broadcast_to(b0, (8, LANE)), jnp.broadcast_to(b1, (8, LANE))))
    gbbuf[r] = by_thirds(pack_gates(packed, unit, npad // LANE), lambda v: dot_t(v, order[...]))
    for k in range(1, R):
        start(gbbuf.at[r], gbbuf.at[r], gbs, gbr, row_dev(lax.rem(r + k, R)))

    wait(x_ref, sbs.at[0])
    wait(xstage, sbs.at[1])
    wait(xstage, sbs.at[2])
    for w in range(3):
        wait(stage.at[w, pl.ds(0, R - 1)], ws.at[w])
    wait(h0.at[pl.ds(0, R - 1)], h0s)
    for cut in range(len(X_CUTS) - 1):
        wait_x(cut, xss)

    @pl.when(owner != me)
    def _():
        wait(c_in, css)

    hflat = hspare.at[pl.ds(0, N - 1)]

    def drain(t, _):
        wait(r1.at[0, pl.ds(0, N - 1)], b1s.at[t])
        wait(zs.at[pl.ds(0, CHIPS - 1), t], zss.at[t])
        wait(hflat, h1s.at[t])

        @pl.when(t < T - 1)
        def _():
            wait(r1.at[0, pl.ds(0, N - 1)], b2s.at[t])
            wait(hflat, h2s.at[t])
        return 0

    lax.fori_loop(0, T, drain, 0)
    place_dz(0)
    wait(gbbuf.at[pl.ds(0, R - 1)], gbr)
    gb_ref[...] = blocks_joined(lambda p: gbbuf[p])
    for layer in range(2):
        for q in range(T // CH):
            wait(dza.at[layer, pl.ds(0, R - 1), pl.ds(0, CH)], dzs.at[layer, q])
    wait(gbbuf.at[pl.ds(0, R - 1)], gbs)


def grad_kernel(left_ref, dzn_ref, gb_ref, gx1, gh1, gx2, gh2, gb1, gb2, buf, sems):
    rows = gx1.shape[0]
    step = rows // GROWS
    copies = []
    for i in range(GROWS):
        for k, (out, layer) in enumerate(((gx1, 0), (gh1, 0), (gx2, 1), (gh2, 1))):
            lo = i * step
            buf[k, lo:lo + step] = dot(left_ref[k, lo:lo + step], dzn_ref[layer])
            copies.append(pltpu.make_async_copy(buf.at[k, pl.ds(lo, step)], out.at[pl.ds(lo, step)], sems.at[k, i]))
            copies[-1].start()
    gb1[...] = gb_ref[0]
    gb2[...] = gb_ref[1]
    for copy in copies:
        copy.wait()


def solution(mesh):
    C, R = mesh.shape['col'], mesh.shape['row']
    N = C * R
    seq_spec = P(None, 'data', 'row')
    w_spec = P('row', 'col')
    bias_spec = P('col')
    g_spec = P(None, 'data', 'col')
    grad_spec = P(('data', 'row'), 'col')
    gbias_spec = P(('data', 'col'))

    def local_grads(seq_in, w_x1, w_h1, w_x2, w_h2, bias_1, bias_2, h_init, c_init, g_out):
        T, B, rows = seq_in.shape
        U = rows * R
        cols = w_x1.shape[1]
        unit = U // N
        npad = -(-4 * unit // LANE) * LANE
        chips = R // 2
        gw = -(-unit * R // LANE) * LANE
        vm = pl.BlockSpec(memory_space=pltpu.VMEM)
        dma = pltpu.SemaphoreType.DMA
        V = pltpu.VMEM
        left, dzn, gb = pl.pallas_call(
            functools.partial(recur_kernel, C, R, T, B, U),
            name='recur',
            out_shape=(jax.ShapeDtypeStruct((4, npad, T * B), BF16), jax.ShapeDtypeStruct((2, T * B, cols), BF16),
                       jax.ShapeDtypeStruct((8, cols), F32)),
            in_specs=[vm] + [pl.BlockSpec(memory_space=pl.ANY)] * 4 + [vm] * 5,
            out_specs=(vm, vm, vm),
            scratch_shapes=[
                V((rows, cols), BF16), V((rows, cols), BF16), V((rows, cols), BF16), V((rows, cols), BF16),
                V((B, cols), F32),
                V((R, WIN, npad), BF16),
                V((3, R, rows, npad), BF16),
                V((chips, rows, npad), BF16),
                V((3, U, npad), BF16),
                V((3, npad, C * gw), BF16),
                V((chips, 2 * rows, npad), BF16),
                V((chips, 2 * rows, npad), BF16),
                V((T, B, rows), BF16),
                V((chips, T, B, npad), F32),
                V((chips, T, B, npad), F32),
                V((chips, T, B, npad), F32),
                V((chips, T, B, npad), F32),
                V((R, 2, B, npad), BF16),
                V((T, C, R, B, LANE), BF16),
                V((T, C, R, B, LANE), BF16),
                V((2, T, 6, B, LANE), F32),
                V((2, B, LANE), F32),
                V((2, B, LANE), F32),
                V((2, B, LANE), F32),
                V((2, B, npad), F32),
                V((T, B, LANE), F32),
                V((B, LANE), F32),
                V((T, N, B, LANE), F32),
                V((T, N, B, LANE), F32),
                V((T, C, R, B, LANE), F32),
                V((T, C, R, B, LANE), F32),
                V((2, T, B, npad), BF16),
                V((2, R, T, B, npad), BF16),
                V((2, 4, B, LANE), F32),
                V((R, 8, npad), F32),
                V((B, C * gw), F32),
                V((B, npad), F32),
                V((2, B, LANE), F32),
                V((B, npad), BF16),
                V((N, B, LANE), BF16),
                dma((4,)),
                dma((3,)), dma((3,)), dma((3,)), dma((3,)), dma((len(X_CUTS) - 1,)), dma((len(X_CUTS) - 1,)), dma((T,)), dma((T,)),
                dma, dma, dma, dma,
                dma((T,)), dma((T, C)), dma((T,)), dma((T, C)),
                dma((T,)), dma((T,)), dma((T,)), dma((T,)),
                dma((2, T // CH)), dma((2, T // CH)), dma, dma,
            ],
            compiler_params=pltpu.CompilerParams(collective_id=0, has_side_effects=True, vmem_limit_bytes=63 * 1024 * 1024),
        )(seq_in, w_x1, w_h1, w_x2, w_h2, bias_1, bias_2, h_init, c_init, g_out)

        out = jax.ShapeDtypeStruct((rows, cols), F32)
        bout = jax.ShapeDtypeStruct((cols,), F32)
        hbm = pl.BlockSpec(memory_space=pl.ANY)
        return tuple(pl.pallas_call(
            grad_kernel,
            name='grads',
            out_shape=(out,) * 4 + (bout,) * 2,
            in_specs=[vm] * 3,
            out_specs=(hbm,) * 4 + (vm,) * 2,
            scratch_shapes=[V((4, rows, cols), F32), dma((4, GROWS))],
            compiler_params=pltpu.CompilerParams(vmem_limit_bytes=40 * 1024 * 1024),
        )(left, dzn, gb))

    return jax.shard_map(local_grads, mesh=mesh,
                         in_specs=(seq_spec, w_spec, w_spec, w_spec, w_spec, bias_spec, bias_spec, seq_spec, seq_spec, g_spec),
                         out_specs=(grad_spec, grad_spec, grad_spec, grad_spec, gbias_spec, gbias_spec),
                         check_vma=False)
```

```python
import functools

import jax
import jax.numpy as jnp
from jax import lax
from jax.experimental import pallas as pl
from jax.experimental.pallas import tpu as pltpu
from jax.sharding import PartitionSpec as P

MESH = pl.DeviceIdType.MESH
F32 = jnp.float32
BF16 = jnp.bfloat16
LANE = 128
WIN = 512
CH = 4
X_CUTS = (0, 4, 8, 12, 16)
X_SEND = (None, 1, 3, 5)
W2_CUTS = (0, 128, 240, 352)
GROWS = 4
WROWS = 32
W_FROM = 4


def dot(a, b):
    return jnp.dot(a, b, preferred_element_type=F32)


def dot_t(a, b):
    return lax.dot_general(a, b, (((1,), (1,)), ((), ())), preferred_element_type=F32)


def by_thirds(x, f):
    x = x * 0.25
    hi = x.astype(BF16)
    rest = x - hi.astype(F32)
    mid = rest.astype(BF16)
    lo = (rest - mid.astype(F32)).astype(BF16)
    return ((f(hi) + f(mid)) + f(lo)) * 4.0


def loop(n, body):
    def step(i, carry):
        body(i, carry)
        return carry
    lax.fori_loop(0, n, step, 0)


def lane_iota(rows):
    return lax.broadcasted_iota(jnp.int32, (rows, LANE), 1)


def join(segs, width):
    lane = lane_iota(segs[0][1].shape[0])
    tiles = []
    for lo in range(0, width, LANE):
        val = None
        for i, (start, tile) in enumerate(segs):
            end = segs[i + 1][0] if i + 1 < len(segs) else width
            if end <= lo or start >= lo + LANE:
                continue
            val = tile if val is None else jnp.where(lane >= start - lo, tile, val)
        tiles.append(val)
    return jnp.concatenate(tiles, axis=1)


def split_gates(z, unit):
    lane = lane_iota(z.shape[0])
    tiles = [z[:, q * LANE:(q + 1) * LANE] for q in range(z.shape[1] // LANE)]
    out = []
    for k in range(4):
        q, s = divmod(k * unit, LANE)
        a = tiles[q]
        if s:
            a = pltpu.roll(a, LANE - s, 1)
            if s + unit > LANE:
                a = jnp.where(lane < LANE - s, a, pltpu.roll(tiles[q + 1], LANE - s, 1))
        out.append(a)
    return out


def pack_gates(parts, unit, n_tiles):
    lane = lane_iota(parts[0].shape[0])
    rolled = [p if (k * unit) % LANE == 0 else pltpu.roll(p, (k * unit) % LANE, 1) for k, p in enumerate(parts)]
    tiles = []
    for q in range(n_tiles):
        val = jnp.zeros_like(parts[0])
        for k in range(4):
            a, b = k * unit - q * LANE, (k + 1) * unit - q * LANE
            if b > 0 and a < LANE:
                val = jnp.where((lane >= a) & (lane < b), rolled[k], val)
        tiles.append(val)
    return jnp.concatenate(tiles, axis=1)


def recur_kernel(C, R, T, B, U,
                 x_ref, wx1_ref, wh1_ref, wx2_ref, wh2_ref, b1_ref, b2_ref, hi_ref, ci_ref, g_ref,
                 left_out, dzn_out, gb_out,
                 left_ref, dzn_ref, gb_ref,
                 wx1, wh1, wx2, wh2, brow, pm, stage, xstage, wf, wt, wc1, wc2, xsib, xs, xr, zs, zr, h0, hist1, hist2, sv, c_out, c_in, cst,
                 bias, gs, part, r1, r2, s1, s2, dzo, dza, gbacc, gbbuf, pxs, zscr, dcs, d1, hspare, zh, zhr, ins, outs, zhs,
                 ws, wr, sbs, sbr, xss, xrs, zss, zrs, h0s, h0r, css, crs, h1s, h1r, h2s, h2r,
                 b1s, b1r, b2s, b2r, dzs, dzr, gbs, gbr):
    N = C * R
    CHIPS = R // 2
    unit = U // N
    rows = U // R
    cols = 4 * U // C
    ncol = 4 * unit
    npad = stage.shape[-1]
    c = lax.axis_index('col')
    r = lax.axis_index('row')
    me = c * R + r
    chip, core = r // 2, lax.rem(r, 2)
    sib = {'col': c, 'row': chip * 2 + 1 - core}
    my_s = lax.rem(r * unit, LANE)
    group = unit * R
    gw = -(-group // LANE) * LANE
    ring = lambda o, n: min(o, n - o)
    far_y = sorted(range(C), key=lambda o: -ring(o, C))
    far_row = sorted(((dx, dk) for dx in range(CHIPS) for dk in range(2)), key=lambda o: -ring(o[0], CHIPS))

    def col_at(dy):
        return lax.rem(c + dy, C)

    def row_at(dx, dk):
        return 2 * lax.rem(chip + dx, CHIPS) + lax.rem(core + dk, 2)

    peers = [(dy, dx, dk) for dy in range(C) for dx, dk in far_row if (dy, dx, dk) != (0, 0, 0)]
    peers.sort(key=lambda o: (not (o[0] and o[1]), -(ring(o[0], C) + ring(o[1], CHIPS))))

    loads = [pltpu.make_async_copy(a, b, ins.at[i]) for i, (a, b) in
             enumerate(((wh1_ref, wh1), (wx1_ref, wx1), (wh2_ref, wh2), (wx2_ref, wx2)))]
    for load in loads:
        load.start()

    others_r, others_n, others_c = (pl.ds(0, n - 1) for n in (R, N, CHIPS))

    def dev(p):
        return {'col': p // R, 'row': lax.rem(p, R)}

    def row_dev(p):
        return {'col': c, 'row': p}

    bar = pltpu.get_barrier_semaphore()
    for k in range(1, N):
        pl.semaphore_signal(bar, inc=1, device_id=dev(lax.rem(me + k, N)), device_id_type=MESH)

    def start(src, dst, ss, rs, did):
        pltpu.make_async_remote_copy(src_ref=src, dst_ref=dst, send_sem=ss, recv_sem=rs, device_id=did, device_id_type=MESH).start()

    def wait(ref, sem):
        pltpu.make_async_copy(ref, ref, sem).wait()

    def win(p):
        return pl.multiple_of(jnp.minimum((p * ncol) // LANE * LANE, cols - WIN), LANE)

    kk = lax.broadcasted_iota(jnp.int32, (WIN, npad), 0)
    nn = lax.broadcasted_iota(jnp.int32, (WIN, npad), 1)
    gate = (nn >= unit).astype(jnp.int32) + (nn >= 2 * unit).astype(jnp.int32) + (nn >= 3 * unit).astype(jnp.int32)
    target = jnp.where(nn < ncol, 4 * (nn - unit * gate) + gate, -cols) - kk

    def regroup(w, p):
        return dot(w[:, pl.ds(win(p), WIN)], pm[p]).astype(BF16)

    def row_block(p):
        return pl.ds(pl.multiple_of(p * rows, 16), rows)

    def make_pm(p, _):
        pm[p] = jnp.where(target == win(p) - p * ncol, 1.0, 0.0).astype(BF16)

    h0[r] = jnp.concatenate([hi_ref[...], jnp.zeros((2, B, npad - rows), F32)], axis=2).astype(BF16)
    loop(R, make_pm)
    pl.semaphore_wait(bar, N - 1)
    start(x_ref, xsib, sbs.at[0], sbr.at[0], sib)
    for dx, dk in far_row:
        if (dx, dk) != (0, 0):
            start(h0.at[r], h0.at[r], h0s, h0r, row_dev(row_at(dx, dk)))
    loads[0].wait()

    def send_h1(k, _):
        p = lax.rem(r + R // 2 + k, R)
        stage[0, p] = regroup(wh1, p)

        @pl.when(p != r)
        def _():
            start(stage.at[0, p], wf.at[0, row_block(r)], ws.at[0], wr.at[0], row_dev(p))

    loop(R, send_h1)
    wf[0, row_block(r)] = stage[0, r]

    def send_h2(cut):
        lo, hi = W2_CUTS[cut], W2_CUTS[cut + 1]
        for dx, dk in far_row:
            if (dx, dk) != (0, 0):
                p = row_at(dx, dk)
                start(stage.at[1, p, pl.ds(lo, hi - lo)], wf.at[1, pl.ds(pl.multiple_of(r * rows + lo, 16), hi - lo)],
                      ws.at[1], wr.at[1], row_dev(p))

    owner = r * (N // R) + c
    ci = jnp.concatenate([ci_ref[...].reshape(2 * B, rows), jnp.zeros((2 * B, npad - rows), F32)], axis=1)
    lane2 = lane_iota(2 * B)
    for j in range(C):
        q, s = divmod(j * unit, LANE)
        v = ci[:, q * LANE:(q + 1) * LANE]
        if s:
            v = pltpu.roll(v, LANE - s, 1)
            if s + unit > LANE:
                v = jnp.where(lane2 < LANE - s, v, pltpu.roll(ci[:, (q + 1) * LANE:(q + 2) * LANE], LANE - s, 1))
        v = jnp.where(lane2 < unit, v, 0.0).reshape(2, B, LANE)

        @pl.when(c == j)
        def _():
            c_out[...] = v

    @pl.when(owner != me)
    def _():
        start(c_out, c_in, css, crs, dev(owner))

    @pl.when(owner == me)
    def _():
        c_in[...] = c_out[...]

    def trade1(j, _):
        mine, other = 2 * j + core, 2 * j + 1 - core
        wc1[j, row_block(core)] = regroup(wx1, mine)
        xstage[j] = regroup(wx1, other)
        start(xstage.at[j], wc1.at[j, row_block(core)], sbs.at[1], sbr.at[1], sib)

    loads[1].wait()
    loop(CHIPS, trade1)
    loads[2].wait()

    def stage_h2(k, _):
        p = lax.rem(r + R // 2 + k, R)
        stage[1, p] = regroup(wh2, p)
        zh[p] = dot(h0[r, 1][:, :rows], stage[1, p])

        @pl.when(p != r)
        def _():
            start(zh.at[p], zhr.at[r], zhs.at[0], zhs.at[1], row_dev(p))

    loop(R, stage_h2)
    zhr[r] = zh[r]
    wait(xsib, sbr.at[0])
    wait(xstage, sbr.at[1])

    def flat(v):
        return v.astype(F32).reshape(T * B, rows).astype(BF16)

    def xproj(j, _):
        v = dot(flat(x_ref[...]), wc1[j, row_block(core)]) + dot(flat(xsib[...]), wc1[j, row_block(1 - core)])
        xs[j] = v.reshape(T, B, npad)

    loop(CHIPS, xproj)

    def send_x(cut):
        ts = pl.ds(X_CUTS[cut], X_CUTS[cut + 1] - X_CUTS[cut])
        for k in (2, 1, 3):
            j = lax.rem(chip + k, CHIPS)
            start(xs.at[j, ts], xr.at[chip, ts], xss.at[cut], xrs.at[cut], row_dev(2 * j + core))

    def wait_x(cut, sems):
        wait(xs.at[others_c, pl.ds(X_CUTS[cut], X_CUTS[cut + 1] - X_CUTS[cut])], sems.at[cut])

    send_x(0)
    xr[chip] = xs[chip]
    send_h2(0)
    wf[1, row_block(r)] = stage[1, r]
    loads[3].wait()

    def trade2(j, _):
        mine, other = 2 * j + core, 2 * j + 1 - core
        blk = regroup(wx2, mine)
        stage[2, mine] = blk
        wc2[j, row_block(core)] = blk
        stage[2, other] = regroup(wx2, other)
        start(stage.at[2, other], wc2.at[j, row_block(core)], sbs.at[2], sbr.at[2], sib)

    loop(CHIPS, trade2)
    wf[2, row_block(r)] = stage[2, r]

    for l, ref in enumerate((b1_ref, b2_ref)):
        brow[...] = jnp.broadcast_to(ref[...].reshape(1, cols), (B, cols))
        b = brow[:, pl.ds(win(r), WIN)]
        bias[l] = by_thirds(b, lambda v: dot(v, pm[r]))
    g_w = g_ref.shape[2]
    sel_k = lax.broadcasted_iota(jnp.int32, (g_w, LANE), 0)
    sel_n = lax.broadcasted_iota(jnp.int32, (g_w, LANE), 1)
    sel = jnp.where((sel_k == sel_n + r * unit) & (sel_n < unit), 1.0, 0.0).astype(BF16)
    gs[...] = dot(g_ref[...].astype(F32).reshape(T * B, g_w).astype(BF16), sel).reshape(T, B, LANE)

    def transpose_w(w):
        eye = (lax.broadcasted_iota(jnp.int32, (npad, npad), 0) == lax.broadcasted_iota(jnp.int32, (npad, npad), 1))
        eye = jnp.where(eye, 1.0, 0.0).astype(BF16)

        def body(k, _):
            for off in range(0, group, 256):
                n = min(256, group - off)
                v = dot_t(eye, wf[w, pl.ds(pl.multiple_of(k * group + off, 16), n)]).astype(BF16)
                if off + n == group and gw > group:
                    v = jnp.concatenate([v, jnp.zeros((npad, gw - group), BF16)], axis=1)
                wt[w, :, pl.ds(pl.multiple_of(k * gw + off, LANE), v.shape[1])] = v
        loop(C, body)

    def cell(layer, t, z):
        zi, zf, zg, zo = split_gates(z, unit)
        gi, gf, gg, go = jax.nn.sigmoid(zi), jax.nn.sigmoid(zf), jnp.tanh(zg), jax.nn.sigmoid(zo)
        c_prev = cst[layer]
        c_new = gf * c_prev + gi * gg
        tc = jnp.tanh(c_new)
        cst[layer] = c_new
        for k, v in enumerate((gi, gf, gg, go, c_prev, tc)):
            sv[layer, t, k] = v
        return pltpu.roll(go * tc, my_s, 1).astype(BF16)

    def bcast(hist, t, ss, rs):
        for dy, dx, dk in peers:
            start(hist.at[t, c, r], hist.at[t, c, r], ss.at[t], rs.at[t, c], {'col': col_at(dy), 'row': row_at(dx, dk)})

    def group_h(hist, t, cs):
        return join([(unit * d, hist[t, cs, d].astype(F32)) for d in range(R)], gw)[:, :group].astype(BF16)

    def h_times(hist, t, rs, w):
        def term(cs):
            return dot(group_h(hist, t, cs), wf[w, pl.ds(pl.multiple_of(cs * group, 16), group)])

        wait(hist.at[t, c, others_r], rs.at[t, c])
        z = term(c)
        for dy in range(1, C):
            wait(hist.at[t, col_at(dy), pl.ds(0, R)], rs.at[t, col_at(dy)])
        for dy in range(1, C):
            z = z + term(col_at(dy))
        return z

    def from_h0(layer):
        v = jnp.zeros((B, npad), F32)
        for p in range(R):
            v = v + dot(h0[p, layer][:, :rows], wf[layer, p * rows:(p + 1) * rows])
        return v

    def total(ref, t):
        return (ref[0, t] + ref[1, t]) + (ref[2, t] + ref[3, t])

    def partial_z2(t):
        h = group_h(hist1, t, chip)
        for j in range(CHIPS):
            zs[j, t] = dot(h, wc2[j])
        for k in (2, 1, 3):
            j = lax.rem(chip + k, CHIPS)
            start(zs.at[j, t], zr.at[chip, t], zss.at[t], zrs.at[t], row_dev(2 * j + core))
        zr[chip, t] = zs[chip, t]

    @pl.when(owner != me)
    def _():
        wait(c_in, crs)
    cst[...] = c_in[...]
    wait(h0.at[others_r], h0r)
    wait_x(0, xrs)
    wait(stage.at[0, others_r], wr.at[0])
    hist1[0, c, r] = cell(0, 0, total(xr, 0) + bias[0] + from_h0(0))
    bcast(hist1, 0, h1s, h1r)
    send_h2(1)
    wait(xstage, sbr.at[2])

    n_pieces = rows // WROWS

    def fwd(s, _):
        for cut in range(1, len(X_CUTS) - 1):
            @pl.when(s == X_CUTS[cut] - 1)
            def _():
                wait_x(cut, xrs)

        @pl.when(s < T - 1)
        def _():
            hist1[s + 1, c, r] = cell(0, s + 1, total(xr, s + 1) + bias[0] + h_times(hist1, s, h1r, 0))
            bcast(hist1, s + 1, h1s, h1r)

        @pl.when(s == T - 1)
        def _():
            for dy in range(C):
                cs = col_at(dy)
                wait(hist1.at[s, cs, pl.ds(0, R if dy else R - 1)], h1r.at[s, cs])

        @pl.when(s < T)
        def _():
            partial_z2(s)

        @pl.when(s == 0)
        def _():
            send_h2(2)

        @pl.when(s == 1)
        def _():
            wait(zh.at[others_r], zhs.at[1])
            v = zhr[0]
            for p in range(1, R):
                v = v + zhr[p]
            zscr[...] = v

        @pl.when(s == 2)
        def _():
            wait(stage.at[1, others_r], wr.at[1])

        @pl.when(s > 1)
        def _():
            zscr[...] = h_times(hist2, s - 2, h2r, 1)

        @pl.when(s > 0)
        def _():
            wait(zs.at[others_c, s - 1], zrs.at[s - 1])
            hist2[s - 1, c, r] = cell(1, s - 1, total(zr, s - 1) + bias[1] + zscr[...])

            @pl.when(s < T)
            def _():
                bcast(hist2, s - 1, h2s, h2r)

        for cut in range(1, len(X_CUTS) - 1):
            @pl.when(s == X_SEND[cut])
            def _():
                send_x(cut)

        @pl.when((s >= W_FROM) & (s < W_FROM + n_pieces))
        def _():
            piece = pl.ds(pl.multiple_of((s - W_FROM) * WROWS, WROWS), WROWS)
            dest = pl.ds(pl.multiple_of(r * rows + (s - W_FROM) * WROWS, WROWS), WROWS)
            for k in range(1, R):
                p = lax.rem(r + k, R)
                start(stage.at[2, p, piece], wf.at[2, dest], ws.at[2], wr.at[2], row_dev(p))

        @pl.when(s == 2)
        def _():
            transpose_w(0)

        @pl.when(s == 4)
        def _():
            transpose_w(1)

        @pl.when(s == T - 1)
        def _():
            wait(stage.at[2, others_r], wr.at[2])
            transpose_w(2)

    loop(T + 1, fwd)

    gbacc[...] = jnp.zeros_like(gbacc)
    dcs[...] = jnp.zeros_like(dcs)

    def cell_grad(layer, t, dh):
        gi, gf, gg, go, c_prev, tc = [sv[layer, t, k] for k in range(6)]
        dc = dcs[layer] + dh * go * (1.0 - tc * tc)
        dz = (dc * gg * gi * (1.0 - gi), dc * c_prev * gf * (1.0 - gf), dc * gi * (1.0 - gg * gg), dh * tc * go * (1.0 - go))
        dcs[layer] = dc * gf
        for k in range(4):
            gbacc[layer, k] += dz[k]
        packed = pack_gates(dz, unit, npad // LANE).astype(BF16)
        dzo[layer, t] = packed
        return packed

    lane_b = lane_iota(B)

    def scatter(term, sbuf, rbuf, t, ss, rs):
        for i, dy in enumerate(far_y):
            cs = col_at(dy)
            p = term(pl.ds(pl.multiple_of(cs * gw, LANE), gw))
            tiles = [p[:, q * LANE:(q + 1) * LANE] for q in range(gw // LANE)]
            for d in range(R):
                q, off = divmod(d * unit, LANE)
                v = tiles[q]
                if off + unit > LANE:
                    v = jnp.where(lane_b >= off, v, tiles[q + 1])
                sbuf[t, i, d] = v
            late = [] if dy else [(j, far_y[j], 0, dk) for j in range(C - 1) for dk in range(2)]
            for j, y, dx, dk in [(i, dy, dx, dk) for dx, dk in far_row if dx or not dy] + late:
                if (y, dx, dk) != (0, 0, 0):
                    p = row_at(dx, dk)
                    start(sbuf.at[t, j, p], rbuf.at[t, me], ss.at[t], rs.at[t], {'col': col_at(y), 'row': p})
            if dy == 0:
                rbuf[t, me] = sbuf[t, i, r]

    def reduced(rbuf, t, rs):
        wait(rbuf.at[t, others_n], rs.at[t])
        vals = [rbuf[t, d] for d in range(N)]
        while len(vals) > 1:
            vals = [a + b for a, b in zip(vals[::2], vals[1::2])]
        return pltpu.roll(vals[0], lax.rem(LANE - my_s, LANE), 1)

    order = pm.at[0, pl.ds(0, npad)]

    def send_dz(layer, t):
        @pl.when(lax.rem(t, CH) == 0)
        def _():
            ts = pl.ds(t, CH)
            v = dzo[layer, ts].astype(F32).reshape(CH * B, npad).astype(BF16)
            dza[layer, r, ts] = dot_t(v, order[...]).reshape(CH, B, npad).astype(BF16)
            for k in range(1, R):
                start(dza.at[layer, r, ts], dza.at[layer, r, ts], dzs.at[layer, t // CH], dzr.at[layer, t // CH],
                      row_dev(lax.rem(r + k, R)))

    def blocks_joined(get):
        segs = []
        for p in range(R):
            v = get(p)
            for a in range(npad // LANE):
                tile = v[:, a * LANE:(a + 1) * LANE]
                s = (p * ncol) % LANE
                segs.append((p * ncol + a * LANE, pltpu.roll(tile, s, 1) if s else tile))
        return join(segs, cols)

    def chunk_like(layer):
        return dza.at[layer, others_r, pl.ds(0, CH)]

    def place_dz(q):
        for layer in range(2):
            wait(chunk_like(layer), dzr.at[layer, q])
            v = blocks_joined(lambda p: dza[layer, p, pl.ds(q * CH, CH)].astype(F32).reshape(CH * B, npad))
            at = pl.ds(pl.multiple_of(q * (CH * B), CH * B), CH * B)
            dzn_ref[layer, at] = v.astype(BF16)
            pltpu.make_async_copy(dzn_ref.at[layer, at], dzn_out.at[layer, at], outs.at[1, layer, q]).start()

    shift = core * ((LANE - rows % LANE) % LANE)
    per = R // 2

    def local_rows(hist, count):
        segs = [(unit * d, pltpu.roll(hist[pl.ds(0, count), chip, per * core + d].astype(F32).reshape(count * B, LANE), shift, 1))
                for d in range(per)]
        return join(segs, npad)

    def put_left(i, v):
        for a in range(npad // LANE):
            left_ref[i, a * LANE:(a + 1) * LANE] = v[:, a * LANE:(a + 1) * LANE].T.astype(BF16)

    def wide(v):
        return jnp.concatenate([v, jnp.zeros((v.shape[0], npad - rows), F32)], axis=1)

    def bwd(s, _):
        t = T - 1 - s
        part[...] = gs[t]

        @pl.when(s > 0)
        def _():
            part[...] += reduced(r2, t, b2r)

        dz2 = cell_grad(1, t, part[...])

        @pl.when(t > 0)
        def _():
            scatter(lambda n: dot(dz2, wt[1, :, n]), s2, r2, t - 1, b2s, b2r)

        pxs[...] = dot(dz2, wt[2])
        send_dz(1, t)

        @pl.when(s == 0)
        def _():
            d1[...] = jnp.zeros_like(d1)

        @pl.when(s > 0)
        def _():
            d1[...] = cell_grad(0, t + 1, reduced(r1, t + 1, b1r))

        scatter(lambda n: dot(d1[...], wt[0, :, n]) + pxs[:, n], s1, r1, t, b1s, b1r)

        @pl.when(s > 0)
        def _():
            send_dz(0, t + 1)

        @pl.when((s >= CH + 2) & (lax.rem(s, CH) == 2))
        def _():
            place_dz(T // CH - 1 - (s - CH - 2) // CH)

        @pl.when(s == 1)
        def _():
            put_left(0, wide(x_ref[...].astype(F32).reshape(T * B, rows)))

        @pl.when(s == 2)
        def _():
            h1_rows = local_rows(hist1, T)
            put_left(2, h1_rows)
            first = h0[r, 0].astype(F32)
            put_left(1, jnp.concatenate([first, h1_rows[:(T - 1) * B]], axis=0))

        @pl.when(s == 3)
        def _():
            put_left(3, jnp.concatenate([h0[r, 1].astype(F32), local_rows(hist2, T - 1)], axis=0))
            pltpu.make_async_copy(left_ref, left_out, outs.at[0, 0, 0]).start()

    loop(T, bwd)
    cell_grad(0, 0, reduced(r1, 0, b1r))
    send_dz(0, 0)

    sub = lax.broadcasted_iota(jnp.int32, (8, LANE), 0)
    packed = []
    for k in range(4):
        b0 = jnp.sum(gbacc[0, k], axis=0, keepdims=True)
        b1 = jnp.sum(gbacc[1, k], axis=0, keepdims=True)
        packed.append(jnp.where(sub == 0, jnp.broadcast_to(b0, (8, LANE)), jnp.broadcast_to(b1, (8, LANE))))
    gbbuf[r] = by_thirds(pack_gates(packed, unit, npad // LANE), lambda v: dot_t(v, order[...]))
    for k in range(1, R):
        start(gbbuf.at[r], gbbuf.at[r], gbs, gbr, row_dev(lax.rem(r + k, R)))

    place_dz(0)
    wait(gbbuf.at[others_r], gbr)
    gb_ref[...] = blocks_joined(lambda p: gbbuf[p])
    pltpu.make_async_copy(gb_ref, gb_out, outs.at[0, 1, 0]).start()
    for layer in range(2):
        for q in range(T // CH):
            wait(chunk_like(layer), dzs.at[layer, q])
    wait(gbbuf.at[others_r], gbs)
    wait(x_ref, sbs.at[0])
    wait(xstage, sbs.at[1])
    wait(xstage, sbs.at[2])
    for w in range(3):
        wait(stage.at[w, others_r], ws.at[w])
    wait(h0.at[others_r], h0s)
    wait(zh.at[others_r], zhs.at[0])
    for cut in range(len(X_CUTS) - 1):
        wait_x(cut, xss)

    @pl.when(owner != me)
    def _():
        wait(c_in, css)

    hflat = hspare.at[others_n]

    def drain(t, _):
        wait(r1.at[0, others_n], b1s.at[t])
        wait(zs.at[others_c, t], zss.at[t])
        wait(hflat, h1s.at[t])

        @pl.when(t < T - 1)
        def _():
            wait(r1.at[0, others_n], b2s.at[t])
            wait(hflat, h2s.at[t])

    loop(T, drain)
    wait(left_ref, outs.at[0, 0, 0])
    wait(gb_ref, outs.at[0, 1, 0])
    for layer in range(2):
        for q in range(T // CH):
            wait(dzn_ref.at[layer, pl.ds(0, CH * B)], outs.at[1, layer, q])


def grad_kernel(left_in, dzn_in, gb_in, gx1, gh1, gx2, gh2, gb1, gb2, left_ref, dzn_ref, gb_ref, buf, ins, sems):
    rows = gx1.shape[0]
    step = rows // GROWS
    loads = [pltpu.make_async_copy(left_in, left_ref, ins.at[0]), pltpu.make_async_copy(dzn_in.at[1], dzn_ref.at[1], ins.at[1]),
             pltpu.make_async_copy(dzn_in.at[0], dzn_ref.at[0], ins.at[2]), pltpu.make_async_copy(gb_in, gb_ref, ins.at[3])]
    for load in loads:
        load.start()
    loads[0].wait()
    copies = []
    for layer, grads in ((1, ((2, gx2), (3, gh2))), (0, ((0, gx1), (1, gh1)))):
        loads[2 - layer].wait()
        for i in range(GROWS):
            for k, out in grads:
                lo = i * step
                buf[k, lo:lo + step] = dot(left_ref[k, lo:lo + step], dzn_ref[layer])
                copies.append(pltpu.make_async_copy(buf.at[k, pl.ds(lo, step)], out.at[pl.ds(lo, step)], sems.at[k, i]))
                copies[-1].start()
    loads[3].wait()
    gb1[...] = gb_ref[0]
    gb2[...] = gb_ref[1]
    for copy in copies:
        copy.wait()


def solution(mesh):
    C, R = mesh.shape['col'], mesh.shape['row']
    N = C * R
    seq_spec = P(None, 'data', 'row')
    w_spec = P('row', 'col')
    bias_spec = P('col')
    g_spec = P(None, 'data', 'col')
    grad_spec = P(('data', 'row'), 'col')
    gbias_spec = P(('data', 'col'))

    def local_grads(seq_in, w_x1, w_h1, w_x2, w_h2, bias_1, bias_2, h_init, c_init, g_out):
        T, B, rows = seq_in.shape
        U = rows * R
        cols = w_x1.shape[1]
        unit = U // N
        npad = -(-4 * unit // LANE) * LANE
        chips = R // 2
        gw = -(-unit * R // LANE) * LANE
        vm = pl.BlockSpec(memory_space=pltpu.VMEM)
        hbm = pl.BlockSpec(memory_space=pl.ANY)
        dma = pltpu.SemaphoreType.DMA
        V = pltpu.VMEM
        left, dzn, gb = pl.pallas_call(
            functools.partial(recur_kernel, C, R, T, B, U),
            name='recur',
            out_shape=(jax.ShapeDtypeStruct((4, npad, T * B), BF16), jax.ShapeDtypeStruct((2, T * B, cols), BF16),
                       jax.ShapeDtypeStruct((8, cols), F32)),
            in_specs=[vm] + [pl.BlockSpec(memory_space=pl.ANY)] * 4 + [vm] * 5,
            out_specs=(hbm, hbm, hbm),
            scratch_shapes=[
                V((4, npad, T * B), BF16), V((2, T * B, cols), BF16), V((8, cols), F32),
                V((rows, cols), BF16), V((rows, cols), BF16), V((rows, cols), BF16), V((rows, cols), BF16),
                V((B, cols), F32),
                V((R, WIN, npad), BF16),
                V((3, R, rows, npad), BF16),
                V((chips, rows, npad), BF16),
                V((3, U, npad), BF16),
                V((3, npad, C * gw), BF16),
                V((chips, 2 * rows, npad), BF16),
                V((chips, 2 * rows, npad), BF16),
                V((T, B, rows), BF16),
                V((chips, T, B, npad), F32),
                V((chips, T, B, npad), F32),
                V((chips, T, B, npad), F32),
                V((chips, T, B, npad), F32),
                V((R, 2, B, npad), BF16),
                V((T, C, R, B, LANE), BF16),
                V((T, C, R, B, LANE), BF16),
                V((2, T, 6, B, LANE), F32),
                V((2, B, LANE), F32),
                V((2, B, LANE), F32),
                V((2, B, LANE), F32),
                V((2, B, npad), F32),
                V((T, B, LANE), F32),
                V((B, LANE), F32),
                V((T, N, B, LANE), F32),
                V((T, N, B, LANE), F32),
                V((T, C, R, B, LANE), F32),
                V((T, C, R, B, LANE), F32),
                V((2, T, B, npad), BF16),
                V((2, R, T, B, npad), BF16),
                V((2, 4, B, LANE), F32),
                V((R, 8, npad), F32),
                V((B, C * gw), F32),
                V((B, npad), F32),
                V((2, B, LANE), F32),
                V((B, npad), BF16),
                V((N, B, LANE), BF16),
                V((R, B, npad), F32),
                V((R, B, npad), F32),
                dma((4,)), dma((2, 2, T // CH)), dma((2,)),
                dma((3,)), dma((3,)), dma((3,)), dma((3,)), dma((len(X_CUTS) - 1,)), dma((len(X_CUTS) - 1,)), dma((T,)), dma((T,)),
                dma, dma, dma, dma,
                dma((T,)), dma((T, C)), dma((T,)), dma((T, C)),
                dma((T,)), dma((T,)), dma((T,)), dma((T,)),
                dma((2, T // CH)), dma((2, T // CH)), dma, dma,
            ],
            compiler_params=pltpu.CompilerParams(collective_id=0, has_side_effects=True, vmem_limit_bytes=63 * 1024 * 1024),
        )(seq_in, w_x1, w_h1, w_x2, w_h2, bias_1, bias_2, h_init, c_init, g_out)

        out = jax.ShapeDtypeStruct((rows, cols), F32)
        bout = jax.ShapeDtypeStruct((cols,), F32)
        return tuple(pl.pallas_call(
            grad_kernel,
            name='grads',
            out_shape=(out,) * 4 + (bout,) * 2,
            in_specs=[hbm] * 3,
            out_specs=(hbm,) * 4 + (vm,) * 2,
            scratch_shapes=[V((4, npad, T * B), BF16), V((2, T * B, cols), BF16), V((8, cols), F32),
                            V((4, rows, cols), F32), dma((4,)), dma((4, GROWS))],
            compiler_params=pltpu.CompilerParams(vmem_limit_bytes=63 * 1024 * 1024),
        )(left, dzn, gb))

    return jax.shard_map(local_grads, mesh=mesh,
                         in_specs=(seq_spec, w_spec, w_spec, w_spec, w_spec, bias_spec, bias_spec, seq_spec, seq_spec, g_spec),
                         out_specs=(grad_spec, grad_spec, grad_spec, grad_spec, gbias_spec, gbias_spec),
                         check_vma=False)
```

```python
import functools

import jax
import jax.numpy as jnp
from jax import lax
from jax.experimental import pallas as pl
from jax.experimental.pallas import tpu as pltpu
from jax.sharding import PartitionSpec as P

MESH = pl.DeviceIdType.MESH
F32 = jnp.float32
BF16 = jnp.bfloat16
LANE = 128
WIN = 512
CH = 4
X_CUTS = (0, 4, 8, 12, 16)
X_SEND = (None, 1, 3, 5)
W2_CUTS = (0, 128, 240, 352)
GROWS = 4
WROWS = 32
W_FROM = 4


def dot(a, b):
    return jnp.dot(a, b, preferred_element_type=F32)


def dot_t(a, b):
    return lax.dot_general(a, b, (((1,), (1,)), ((), ())), preferred_element_type=F32)


def by_thirds(x, f):
    x = x * 0.25
    hi = x.astype(BF16)
    rest = x - hi.astype(F32)
    mid = rest.astype(BF16)
    lo = (rest - mid.astype(F32)).astype(BF16)
    return ((f(hi) + f(mid)) + f(lo)) * 4.0


def loop(n, body):
    def step(i, carry):
        body(i, carry)
        return carry
    lax.fori_loop(0, n, step, 0)


def lane_iota(rows):
    return lax.broadcasted_iota(jnp.int32, (rows, LANE), 1)


def join(segs, width):
    lane = lane_iota(segs[0][1].shape[0])
    tiles = []
    for lo in range(0, width, LANE):
        val = None
        for i, (start, tile) in enumerate(segs):
            end = segs[i + 1][0] if i + 1 < len(segs) else width
            if end <= lo or start >= lo + LANE:
                continue
            val = tile if val is None else jnp.where(lane >= start - lo, tile, val)
        tiles.append(val)
    return jnp.concatenate(tiles, axis=1)


def split_gates(z, unit):
    lane = lane_iota(z.shape[0])
    tiles = [z[:, q * LANE:(q + 1) * LANE] for q in range(z.shape[1] // LANE)]
    out = []
    for k in range(4):
        q, s = divmod(k * unit, LANE)
        a = tiles[q]
        if s:
            a = pltpu.roll(a, LANE - s, 1)
            if s + unit > LANE:
                a = jnp.where(lane < LANE - s, a, pltpu.roll(tiles[q + 1], LANE - s, 1))
        out.append(a)
    return out


def pack_gates(parts, unit, n_tiles):
    lane = lane_iota(parts[0].shape[0])
    rolled = [p if (k * unit) % LANE == 0 else pltpu.roll(p, (k * unit) % LANE, 1) for k, p in enumerate(parts)]
    tiles = []
    for q in range(n_tiles):
        val = jnp.zeros_like(parts[0])
        for k in range(4):
            a, b = k * unit - q * LANE, (k + 1) * unit - q * LANE
            if b > 0 and a < LANE:
                val = jnp.where((lane >= a) & (lane < b), rolled[k], val)
        tiles.append(val)
    return jnp.concatenate(tiles, axis=1)


def recur_kernel(C, R, T, B, U,
                 x_ref, wx1_ref, wh1_ref, wx2_ref, wh2_ref, b1_ref, b2_ref, hi_ref, ci_ref, g_ref,
                 left_out, dzn_out, gb_out,
                 left_ref, dzn_ref, gb_ref,
                 wx1, wh1, wx2, wh2, brow, pm, stage, xstage, wf, wt, wc1, wc2, xsib, xs, xr, zs, zr, h0, hist1, hist2, sv, c_out, c_in, cst,
                 bias, gs, part, r1, r2, s1, s2, dzo, dza, gbacc, gbbuf, pxs, zscr, dcs, d1, hspare, zh, zhr, ins, outs, zhs,
                 ws, wr, sbs, sbr, xss, xrs, zss, zrs, h0s, h0r, css, crs, h1s, h1r, h2s, h2r,
                 b1s, b1r, b2s, b2r, dzs, dzr, gbs, gbr):
    N = C * R
    CHIPS = R // 2
    unit = U // N
    rows = U // R
    cols = 4 * U // C
    ncol = 4 * unit
    npad = stage.shape[-1]
    c = lax.axis_index('col')
    r = lax.axis_index('row')
    me = c * R + r
    chip, core = r // 2, lax.rem(r, 2)
    sib = {'col': c, 'row': chip * 2 + 1 - core}
    my_s = lax.rem(r * unit, LANE)
    group = unit * R
    gw = -(-group // LANE) * LANE
    ring = lambda o, n: min(o, n - o)
    far_y = sorted(range(C), key=lambda o: -ring(o, C))
    far_row = sorted(((dx, dk) for dx in range(CHIPS) for dk in range(2)), key=lambda o: -ring(o[0], CHIPS))

    def col_at(dy):
        return lax.rem(c + dy, C)

    def row_at(dx, dk):
        return 2 * lax.rem(chip + dx, CHIPS) + lax.rem(core + dk, 2)

    peers = [(dy, dx, dk) for dy in range(C) for dx, dk in far_row if (dy, dx, dk) != (0, 0, 0)]
    peers.sort(key=lambda o: (not (o[0] and o[1]), -(ring(o[0], C) + ring(o[1], CHIPS))))

    loads = [pltpu.make_async_copy(a, b, ins.at[i]) for i, (a, b) in
             enumerate(((wh1_ref, wh1), (wx1_ref, wx1), (wh2_ref, wh2), (wx2_ref, wx2)))]
    for load in loads:
        load.start()

    others_r, others_n, others_c = (pl.ds(0, n - 1) for n in (R, N, CHIPS))

    def dev(p):
        return {'col': p // R, 'row': lax.rem(p, R)}

    def row_dev(p):
        return {'col': c, 'row': p}

    bar = pltpu.get_barrier_semaphore()
    for k in range(1, N):
        pl.semaphore_signal(bar, inc=1, device_id=dev(lax.rem(me + k, N)), device_id_type=MESH)

    def start(src, dst, ss, rs, did):
        pltpu.make_async_remote_copy(src_ref=src, dst_ref=dst, send_sem=ss, recv_sem=rs, device_id=did, device_id_type=MESH).start()

    def wait(ref, sem):
        pltpu.make_async_copy(ref, ref, sem).wait()

    def win(p):
        return pl.multiple_of(jnp.minimum((p * ncol) // LANE * LANE, cols - WIN), LANE)

    kk = lax.broadcasted_iota(jnp.int32, (WIN, npad), 0)
    nn = lax.broadcasted_iota(jnp.int32, (WIN, npad), 1)
    gate = (nn >= unit).astype(jnp.int32) + (nn >= 2 * unit).astype(jnp.int32) + (nn >= 3 * unit).astype(jnp.int32)
    target = jnp.where(nn < ncol, 4 * (nn - unit * gate) + gate, -cols) - kk

    def regroup(w, p):
        return dot(w[:, pl.ds(win(p), WIN)], pm[p]).astype(BF16)

    def row_block(p):
        return pl.ds(pl.multiple_of(p * rows, 16), rows)

    def make_pm(p, _):
        pm[p] = jnp.where(target == win(p) - p * ncol, 1.0, 0.0).astype(BF16)

    h0[r] = jnp.concatenate([hi_ref[...], jnp.zeros((2, B, npad - rows), F32)], axis=2).astype(BF16)
    loop(R, make_pm)
    pl.semaphore_wait(bar, N - 1)
    start(x_ref, xsib, sbs.at[0], sbr.at[0], sib)
    for dx, dk in far_row:
        if (dx, dk) != (0, 0):
            start(h0.at[r], h0.at[r], h0s, h0r, row_dev(row_at(dx, dk)))
    loads[0].wait()

    def send_h1(k, _):
        p = lax.rem(r + R // 2 + k, R)
        stage[0, p] = regroup(wh1, p)

        @pl.when(p != r)
        def _():
            start(stage.at[0, p], wf.at[0, row_block(r)], ws.at[0], wr.at[0], row_dev(p))

    loop(R, send_h1)
    wf[0, row_block(r)] = stage[0, r]

    def send_h2(cut):
        lo, hi = W2_CUTS[cut], W2_CUTS[cut + 1]
        for dx, dk in far_row:
            if (dx, dk) != (0, 0):
                p = row_at(dx, dk)
                start(stage.at[1, p, pl.ds(lo, hi - lo)], wf.at[1, pl.ds(pl.multiple_of(r * rows + lo, 16), hi - lo)],
                      ws.at[1], wr.at[1], row_dev(p))

    owner = r * (N // R) + c
    ci = jnp.concatenate([ci_ref[...].reshape(2 * B, rows), jnp.zeros((2 * B, npad - rows), F32)], axis=1)
    lane2 = lane_iota(2 * B)
    for j in range(C):
        q, s = divmod(j * unit, LANE)
        v = ci[:, q * LANE:(q + 1) * LANE]
        if s:
            v = pltpu.roll(v, LANE - s, 1)
            if s + unit > LANE:
                v = jnp.where(lane2 < LANE - s, v, pltpu.roll(ci[:, (q + 1) * LANE:(q + 2) * LANE], LANE - s, 1))
        v = jnp.where(lane2 < unit, v, 0.0).reshape(2, B, LANE)

        @pl.when(c == j)
        def _():
            c_out[...] = v

    @pl.when(owner != me)
    def _():
        start(c_out, c_in, css, crs, dev(owner))

    @pl.when(owner == me)
    def _():
        c_in[...] = c_out[...]

    def trade1(j, _):
        mine, other = 2 * j + core, 2 * j + 1 - core
        wc1[j, row_block(core)] = regroup(wx1, mine)
        xstage[j] = regroup(wx1, other)
        start(xstage.at[j], wc1.at[j, row_block(core)], sbs.at[1], sbr.at[1], sib)

    loads[1].wait()
    loop(CHIPS, trade1)
    loads[2].wait()

    def stage_h2(k, _):
        p = lax.rem(r + R // 2 + k, R)
        stage[1, p] = regroup(wh2, p)
        zh[p] = dot(h0[r, 1][:, :rows], stage[1, p])

        @pl.when(p != r)
        def _():
            start(zh.at[p], zhr.at[r], zhs.at[0], zhs.at[1], row_dev(p))

    loop(R, stage_h2)
    zhr[r] = zh[r]
    wait(xsib, sbr.at[0])
    wait(xstage, sbr.at[1])

    def flat(v):
        return v.astype(F32).reshape(T * B, rows).astype(BF16)

    def xproj(j, _):
        v = dot(flat(x_ref[...]), wc1[j, row_block(core)]) + dot(flat(xsib[...]), wc1[j, row_block(1 - core)])
        xs[j] = v.reshape(T, B, npad)

    loop(CHIPS, xproj)

    def send_x(cut):
        ts = pl.ds(X_CUTS[cut], X_CUTS[cut + 1] - X_CUTS[cut])
        for k in (2, 1, 3):
            j = lax.rem(chip + k, CHIPS)
            start(xs.at[j, ts], xr.at[chip, ts], xss.at[cut], xrs.at[cut], row_dev(2 * j + core))

    def wait_x(cut, sems):
        wait(xs.at[others_c, pl.ds(X_CUTS[cut], X_CUTS[cut + 1] - X_CUTS[cut])], sems.at[cut])

    send_x(0)
    xr[chip] = xs[chip]
    send_h2(0)
    wf[1, row_block(r)] = stage[1, r]
    loads[3].wait()

    def trade2(j, _):
        mine, other = 2 * j + core, 2 * j + 1 - core
        blk = regroup(wx2, mine)
        stage[2, mine] = blk
        wc2[j, row_block(core)] = blk
        stage[2, other] = regroup(wx2, other)
        start(stage.at[2, other], wc2.at[j, row_block(core)], sbs.at[2], sbr.at[2], sib)

    loop(CHIPS, trade2)
    wf[2, row_block(r)] = stage[2, r]

    for l, ref in enumerate((b1_ref, b2_ref)):
        brow[...] = jnp.broadcast_to(ref[...].reshape(1, cols), (B, cols))
        b = brow[:, pl.ds(win(r), WIN)]
        bias[l] = by_thirds(b, lambda v: dot(v, pm[r]))
    g_w = g_ref.shape[2]
    sel_k = lax.broadcasted_iota(jnp.int32, (g_w, LANE), 0)
    sel_n = lax.broadcasted_iota(jnp.int32, (g_w, LANE), 1)
    sel = jnp.where((sel_k == sel_n + r * unit) & (sel_n < unit), 1.0, 0.0).astype(BF16)
    gs[...] = dot(g_ref[...].astype(F32).reshape(T * B, g_w).astype(BF16), sel).reshape(T, B, LANE)

    def transpose_w(w):
        eye = (lax.broadcasted_iota(jnp.int32, (npad, npad), 0) == lax.broadcasted_iota(jnp.int32, (npad, npad), 1))
        eye = jnp.where(eye, 1.0, 0.0).astype(BF16)

        def body(k, _):
            for off in range(0, group, 256):
                n = min(256, group - off)
                v = dot_t(eye, wf[w, pl.ds(pl.multiple_of(k * group + off, 16), n)]).astype(BF16)
                if off + n == group and gw > group:
                    v = jnp.concatenate([v, jnp.zeros((npad, gw - group), BF16)], axis=1)
                wt[w, :, pl.ds(pl.multiple_of(k * gw + off, LANE), v.shape[1])] = v
        loop(C, body)

    def cell(layer, t, z):
        zi, zf, zg, zo = split_gates(z, unit)
        gi, gf, gg, go = jax.nn.sigmoid(zi), jax.nn.sigmoid(zf), jnp.tanh(zg), jax.nn.sigmoid(zo)
        c_prev = cst[layer]
        c_new = gf * c_prev + gi * gg
        tc = jnp.tanh(c_new)
        cst[layer] = c_new
        for k, v in enumerate((gi, gf, gg, go, c_prev, tc)):
            sv[layer, t, k] = v
        return pltpu.roll(go * tc, my_s, 1).astype(BF16)

    def bcast(hist, t, ss, rs):
        for dy, dx, dk in peers:
            start(hist.at[t, c, r], hist.at[t, c, r], ss.at[t], rs.at[t, c], {'col': col_at(dy), 'row': row_at(dx, dk)})

    def group_h(hist, t, cs):
        return join([(unit * d, hist[t, cs, d].astype(F32)) for d in range(R)], gw)[:, :group].astype(BF16)

    def h_times(hist, t, rs, w):
        def term(cs):
            return dot(group_h(hist, t, cs), wf[w, pl.ds(pl.multiple_of(cs * group, 16), group)])

        wait(hist.at[t, c, others_r], rs.at[t, c])
        z = term(c)
        for dy in range(1, C):
            wait(hist.at[t, col_at(dy), pl.ds(0, R)], rs.at[t, col_at(dy)])
        for dy in range(1, C):
            z = z + term(col_at(dy))
        return z

    def from_h0(layer):
        v = jnp.zeros((B, npad), F32)
        for p in range(R):
            v = v + dot(h0[p, layer][:, :rows], wf[layer, p * rows:(p + 1) * rows])
        return v

    def total(ref, t):
        return (ref[0, t] + ref[1, t]) + (ref[2, t] + ref[3, t])

    def partial_z2(t):
        h = group_h(hist1, t, chip)
        for j in range(CHIPS):
            zs[j, t] = dot(h, wc2[j])
        for k in (2, 1, 3):
            j = lax.rem(chip + k, CHIPS)
            start(zs.at[j, t], zr.at[chip, t], zss.at[t], zrs.at[t], row_dev(2 * j + core))
        zr[chip, t] = zs[chip, t]

    @pl.when(owner != me)
    def _():
        wait(c_in, crs)
    cst[...] = c_in[...]
    wait(h0.at[others_r], h0r)
    wait_x(0, xrs)
    wait(stage.at[0, others_r], wr.at[0])
    hist1[0, c, r] = cell(0, 0, total(xr, 0) + bias[0] + from_h0(0))
    bcast(hist1, 0, h1s, h1r)
    send_h2(1)
    wait(xstage, sbr.at[2])

    n_pieces = rows // WROWS

    def fwd(s, _):
        for cut in range(1, len(X_CUTS) - 1):
            @pl.when(s == X_CUTS[cut] - 1)
            def _():
                wait_x(cut, xrs)

        @pl.when(s < T - 1)
        def _():
            hist1[s + 1, c, r] = cell(0, s + 1, total(xr, s + 1) + bias[0] + h_times(hist1, s, h1r, 0))
            bcast(hist1, s + 1, h1s, h1r)

        @pl.when(s == T - 1)
        def _():
            for dy in range(C):
                cs = col_at(dy)
                wait(hist1.at[s, cs, pl.ds(0, R if dy else R - 1)], h1r.at[s, cs])

        @pl.when(s < T)
        def _():
            partial_z2(s)

        @pl.when(s == 0)
        def _():
            send_h2(2)

        @pl.when(s == 1)
        def _():
            wait(zh.at[others_r], zhs.at[1])
            v = zhr[0]
            for p in range(1, R):
                v = v + zhr[p]
            zscr[...] = v

        @pl.when(s == 2)
        def _():
            wait(stage.at[1, others_r], wr.at[1])

        @pl.when(s > 1)
        def _():
            zscr[...] = h_times(hist2, s - 2, h2r, 1)

        @pl.when(s > 0)
        def _():
            wait(zs.at[others_c, s - 1], zrs.at[s - 1])
            hist2[s - 1, c, r] = cell(1, s - 1, total(zr, s - 1) + bias[1] + zscr[...])

            @pl.when(s < T)
            def _():
                bcast(hist2, s - 1, h2s, h2r)

        for cut in range(1, len(X_CUTS) - 1):
            @pl.when(s == X_SEND[cut])
            def _():
                send_x(cut)

        @pl.when((s >= W_FROM) & (s < W_FROM + n_pieces))
        def _():
            piece = pl.ds(pl.multiple_of((s - W_FROM) * WROWS, WROWS), WROWS)
            dest = pl.ds(pl.multiple_of(r * rows + (s - W_FROM) * WROWS, WROWS), WROWS)
            for k in range(1, R):
                p = lax.rem(r + k, R)
                start(stage.at[2, p, piece], wf.at[2, dest], ws.at[2], wr.at[2], row_dev(p))

        @pl.when(s == 2)
        def _():
            transpose_w(0)

        @pl.when(s == 4)
        def _():
            transpose_w(1)

        @pl.when(s == T - 1)
        def _():
            wait(stage.at[2, others_r], wr.at[2])
            transpose_w(2)

    loop(T + 1, fwd)

    gbacc[...] = jnp.zeros_like(gbacc)
    dcs[...] = jnp.zeros_like(dcs)

    def cell_grad(layer, t, dh):
        gi, gf, gg, go, c_prev, tc = [sv[layer, t, k] for k in range(6)]
        dc = dcs[layer] + dh * go * (1.0 - tc * tc)
        dz = (dc * gg * gi * (1.0 - gi), dc * c_prev * gf * (1.0 - gf), dc * gi * (1.0 - gg * gg), dh * tc * go * (1.0 - go))
        dcs[layer] = dc * gf
        for k in range(4):
            gbacc[layer, k] += dz[k]
        packed = pack_gates(dz, unit, npad // LANE).astype(BF16)
        dzo[layer, t] = packed
        return packed

    lane_b = lane_iota(B)

    def scatter(term, sbuf, rbuf, t, ss, rs):
        for i, dy in enumerate(far_y):
            cs = col_at(dy)
            p = term(pl.ds(pl.multiple_of(cs * gw, LANE), gw))
            tiles = [p[:, q * LANE:(q + 1) * LANE] for q in range(gw // LANE)]
            for d in range(R):
                q, off = divmod(d * unit, LANE)
                v = tiles[q]
                if off + unit > LANE:
                    v = jnp.where(lane_b >= off, v, tiles[q + 1])
                sbuf[t, i, d] = v
            late = [] if dy else [(j, far_y[j], 0, dk) for j in range(C - 1) for dk in range(2)]
            for j, y, dx, dk in [(i, dy, dx, dk) for dx, dk in far_row if dx or not dy] + late:
                if (y, dx, dk) != (0, 0, 0):
                    p = row_at(dx, dk)
                    start(sbuf.at[t, j, p], rbuf.at[t, me], ss.at[t], rs.at[t], {'col': col_at(y), 'row': p})
            if dy == 0:
                rbuf[t, me] = sbuf[t, i, r]

    def reduced(rbuf, t, rs):
        wait(rbuf.at[t, others_n], rs.at[t])
        vals = [rbuf[t, d] for d in range(N)]
        while len(vals) > 1:
            vals = [a + b for a, b in zip(vals[::2], vals[1::2])]
        return pltpu.roll(vals[0], lax.rem(LANE - my_s, LANE), 1)

    order = pm.at[0, pl.ds(0, npad)]

    def send_dz(layer, t):
        @pl.when(lax.rem(t, CH) == 0)
        def _():
            ts = pl.ds(t, CH)
            v = dzo[layer, ts].astype(F32).reshape(CH * B, npad).astype(BF16)
            dza[layer, r, ts] = dot_t(v, order[...]).reshape(CH, B, npad).astype(BF16)
            for k in range(1, R):
                start(dza.at[layer, r, ts], dza.at[layer, r, ts], dzs.at[layer, t // CH], dzr.at[layer, t // CH],
                      row_dev(lax.rem(r + k, R)))

    def blocks_joined(get):
        segs = []
        for p in range(R):
            v = get(p)
            for a in range(npad // LANE):
                tile = v[:, a * LANE:(a + 1) * LANE]
                s = (p * ncol) % LANE
                segs.append((p * ncol + a * LANE, pltpu.roll(tile, s, 1) if s else tile))
        return join(segs, cols)

    def chunk_like(layer):
        return dza.at[layer, others_r, pl.ds(0, CH)]

    def place_dz(q, layers=(1, 0)):
        for layer in layers:
            wait(chunk_like(layer), dzr.at[layer, q])
            v = blocks_joined(lambda p: dza[layer, p, pl.ds(q * CH, CH)].astype(F32).reshape(CH * B, npad))
            at = pl.ds(pl.multiple_of(q * (CH * B), CH * B), CH * B)
            dzn_ref[layer, at] = v.astype(BF16)
            pltpu.make_async_copy(dzn_ref.at[layer, at], dzn_out.at[layer, at], outs.at[1, layer, q]).start()

    shift = core * ((LANE - rows % LANE) % LANE)
    per = R // 2

    def local_rows(hist, count):
        segs = [(unit * d, pltpu.roll(hist[pl.ds(0, count), chip, per * core + d].astype(F32).reshape(count * B, LANE), shift, 1))
                for d in range(per)]
        return join(segs, npad)

    def put_left(i, v):
        for a in range(npad // LANE):
            left_ref[i, a * LANE:(a + 1) * LANE] = v[:, a * LANE:(a + 1) * LANE].T.astype(BF16)

    def wide(v):
        return jnp.concatenate([v, jnp.zeros((v.shape[0], npad - rows), F32)], axis=1)

    def bwd(s, _):
        t = T - 1 - s
        part[...] = gs[t]

        @pl.when(s > 0)
        def _():
            part[...] += reduced(r2, t, b2r)

        dz2 = cell_grad(1, t, part[...])

        @pl.when(t > 0)
        def _():
            scatter(lambda n: dot(dz2, wt[1, :, n]), s2, r2, t - 1, b2s, b2r)

        pxs[...] = dot(dz2, wt[2])
        send_dz(1, t)

        @pl.when(s == 0)
        def _():
            d1[...] = jnp.zeros_like(d1)

        @pl.when(s > 0)
        def _():
            d1[...] = cell_grad(0, t + 1, reduced(r1, t + 1, b1r))

        scatter(lambda n: dot(d1[...], wt[0, :, n]) + pxs[:, n], s1, r1, t, b1s, b1r)

        @pl.when(s > 0)
        def _():
            send_dz(0, t + 1)

        @pl.when((s >= CH + 2) & (lax.rem(s, CH) == 2))
        def _():
            place_dz(T // CH - 1 - (s - CH - 2) // CH)

        @pl.when(s == 1)
        def _():
            put_left(0, wide(x_ref[...].astype(F32).reshape(T * B, rows)))

        @pl.when(s == 2)
        def _():
            h1_rows = local_rows(hist1, T)
            put_left(2, h1_rows)
            first = h0[r, 0].astype(F32)
            put_left(1, jnp.concatenate([first, h1_rows[:(T - 1) * B]], axis=0))

        @pl.when(s == 3)
        def _():
            put_left(3, jnp.concatenate([h0[r, 1].astype(F32), local_rows(hist2, T - 1)], axis=0))
            pltpu.make_async_copy(left_ref, left_out, outs.at[0, 0, 0]).start()

    loop(T, bwd)
    place_dz(0, (1,))
    cell_grad(0, 0, reduced(r1, 0, b1r))
    send_dz(0, 0)

    sub = lax.broadcasted_iota(jnp.int32, (8, LANE), 0)
    packed = []
    for k in range(4):
        b0 = jnp.sum(gbacc[0, k], axis=0, keepdims=True)
        b1 = jnp.sum(gbacc[1, k], axis=0, keepdims=True)
        packed.append(jnp.where(sub == 0, jnp.broadcast_to(b0, (8, LANE)), jnp.broadcast_to(b1, (8, LANE))))
    gbbuf[r] = by_thirds(pack_gates(packed, unit, npad // LANE), lambda v: dot_t(v, order[...]))
    for k in range(1, R):
        start(gbbuf.at[r], gbbuf.at[r], gbs, gbr, row_dev(lax.rem(r + k, R)))

    place_dz(0, (0,))
    wait(gbbuf.at[others_r], gbr)
    gb_ref[...] = blocks_joined(lambda p: gbbuf[p])
    pltpu.make_async_copy(gb_ref, gb_out, outs.at[0, 1, 0]).start()
    for layer in range(2):
        for q in range(T // CH):
            wait(chunk_like(layer), dzs.at[layer, q])
    wait(gbbuf.at[others_r], gbs)
    wait(x_ref, sbs.at[0])
    wait(xstage, sbs.at[1])
    wait(xstage, sbs.at[2])
    for w in range(3):
        wait(stage.at[w, others_r], ws.at[w])
    wait(h0.at[others_r], h0s)
    wait(zh.at[others_r], zhs.at[0])
    for cut in range(len(X_CUTS) - 1):
        wait_x(cut, xss)

    @pl.when(owner != me)
    def _():
        wait(c_in, css)

    hflat = hspare.at[others_n]

    def drain(t, _):
        wait(r1.at[0, others_n], b1s.at[t])
        wait(zs.at[others_c, t], zss.at[t])
        wait(hflat, h1s.at[t])

        @pl.when(t < T - 1)
        def _():
            wait(r1.at[0, others_n], b2s.at[t])
            wait(hflat, h2s.at[t])

    loop(T, drain)
    wait(left_ref, outs.at[0, 0, 0])
    wait(gb_ref, outs.at[0, 1, 0])
    for layer in range(2):
        for q in range(T // CH):
            wait(dzn_ref.at[layer, pl.ds(0, CH * B)], outs.at[1, layer, q])


def grad_kernel(left_in, dzn_in, gb_in, gx1, gh1, gx2, gh2, gb1, gb2, left_ref, dzn_ref, gb_ref, buf, ins, sems):
    rows = gx1.shape[0]
    step = rows // GROWS
    loads = [pltpu.make_async_copy(left_in, left_ref, ins.at[0]), pltpu.make_async_copy(dzn_in.at[1], dzn_ref.at[1], ins.at[1]),
             pltpu.make_async_copy(dzn_in.at[0], dzn_ref.at[0], ins.at[2]), pltpu.make_async_copy(gb_in, gb_ref, ins.at[3])]
    for load in loads:
        load.start()
    loads[0].wait()
    copies = []
    for layer, grads in ((1, ((2, gx2), (3, gh2))), (0, ((0, gx1), (1, gh1)))):
        loads[2 - layer].wait()
        for i in range(GROWS):
            for k, out in grads:
                lo = i * step
                buf[k, lo:lo + step] = dot(left_ref[k, lo:lo + step], dzn_ref[layer])
                copies.append(pltpu.make_async_copy(buf.at[k, pl.ds(lo, step)], out.at[pl.ds(lo, step)], sems.at[k, i]))
                copies[-1].start()
    loads[3].wait()
    gb1[...] = gb_ref[0]
    gb2[...] = gb_ref[1]
    for copy in copies:
        copy.wait()


def solution(mesh):
    C, R = mesh.shape['col'], mesh.shape['row']
    N = C * R
    seq_spec = P(None, 'data', 'row')
    w_spec = P('row', 'col')
    bias_spec = P('col')
    g_spec = P(None, 'data', 'col')
    grad_spec = P(('data', 'row'), 'col')
    gbias_spec = P(('data', 'col'))

    def local_grads(seq_in, w_x1, w_h1, w_x2, w_h2, bias_1, bias_2, h_init, c_init, g_out):
        T, B, rows = seq_in.shape
        U = rows * R
        cols = w_x1.shape[1]
        unit = U // N
        npad = -(-4 * unit // LANE) * LANE
        chips = R // 2
        gw = -(-unit * R // LANE) * LANE
        vm = pl.BlockSpec(memory_space=pltpu.VMEM)
        hbm = pl.BlockSpec(memory_space=pl.ANY)
        dma = pltpu.SemaphoreType.DMA
        V = pltpu.VMEM
        left, dzn, gb = pl.pallas_call(
            functools.partial(recur_kernel, C, R, T, B, U),
            name='recur',
            out_shape=(jax.ShapeDtypeStruct((4, npad, T * B), BF16), jax.ShapeDtypeStruct((2, T * B, cols), BF16),
                       jax.ShapeDtypeStruct((8, cols), F32)),
            in_specs=[vm] + [pl.BlockSpec(memory_space=pl.ANY)] * 4 + [vm] * 5,
            out_specs=(hbm, hbm, hbm),
            scratch_shapes=[
                V((4, npad, T * B), BF16), V((2, T * B, cols), BF16), V((8, cols), F32),
                V((rows, cols), BF16), V((rows, cols), BF16), V((rows, cols), BF16), V((rows, cols), BF16),
                V((B, cols), F32),
                V((R, WIN, npad), BF16),
                V((3, R, rows, npad), BF16),
                V((chips, rows, npad), BF16),
                V((3, U, npad), BF16),
                V((3, npad, C * gw), BF16),
                V((chips, 2 * rows, npad), BF16),
                V((chips, 2 * rows, npad), BF16),
                V((T, B, rows), BF16),
                V((chips, T, B, npad), F32),
                V((chips, T, B, npad), F32),
                V((chips, T, B, npad), F32),
                V((chips, T, B, npad), F32),
                V((R, 2, B, npad), BF16),
                V((T, C, R, B, LANE), BF16),
                V((T, C, R, B, LANE), BF16),
                V((2, T, 6, B, LANE), F32),
                V((2, B, LANE), F32),
                V((2, B, LANE), F32),
                V((2, B, LANE), F32),
                V((2, B, npad), F32),
                V((T, B, LANE), F32),
                V((B, LANE), F32),
                V((T, N, B, LANE), F32),
                V((T, N, B, LANE), F32),
                V((T, C, R, B, LANE), F32),
                V((T, C, R, B, LANE), F32),
                V((2, T, B, npad), BF16),
                V((2, R, T, B, npad), BF16),
                V((2, 4, B, LANE), F32),
                V((R, 8, npad), F32),
                V((B, C * gw), F32),
                V((B, npad), F32),
                V((2, B, LANE), F32),
                V((B, npad), BF16),
                V((N, B, LANE), BF16),
                V((R, B, npad), F32),
                V((R, B, npad), F32),
                dma((4,)), dma((2, 2, T // CH)), dma((2,)),
                dma((3,)), dma((3,)), dma((3,)), dma((3,)), dma((len(X_CUTS) - 1,)), dma((len(X_CUTS) - 1,)), dma((T,)), dma((T,)),
                dma, dma, dma, dma,
                dma((T,)), dma((T, C)), dma((T,)), dma((T, C)),
                dma((T,)), dma((T,)), dma((T,)), dma((T,)),
                dma((2, T // CH)), dma((2, T // CH)), dma, dma,
            ],
            compiler_params=pltpu.CompilerParams(collective_id=0, has_side_effects=True, vmem_limit_bytes=63 * 1024 * 1024),
        )(seq_in, w_x1, w_h1, w_x2, w_h2, bias_1, bias_2, h_init, c_init, g_out)

        out = jax.ShapeDtypeStruct((rows, cols), F32)
        bout = jax.ShapeDtypeStruct((cols,), F32)
        return tuple(pl.pallas_call(
            grad_kernel,
            name='grads',
            out_shape=(out,) * 4 + (bout,) * 2,
            in_specs=[hbm] * 3,
            out_specs=(hbm,) * 4 + (vm,) * 2,
            scratch_shapes=[V((4, npad, T * B), BF16), V((2, T * B, cols), BF16), V((8, cols), F32),
                            V((4, rows, cols), F32), dma((4,)), dma((4, GROWS))],
            compiler_params=pltpu.CompilerParams(vmem_limit_bytes=63 * 1024 * 1024),
        )(left, dzn, gb))

    return jax.shard_map(local_grads, mesh=mesh,
                         in_specs=(seq_spec, w_spec, w_spec, w_spec, w_spec, bias_spec, bias_spec, seq_spec, seq_spec, g_spec),
                         out_specs=(grad_spec, grad_spec, grad_spec, grad_spec, gbias_spec, gbias_spec),
                         check_vma=False)
```
